32 devices in a mesh: dp: 2 (over x), tp: 16 (over y, z, core).
Axes of the slice: x: 2, y: 2, z: 4, core: 2. Of those that a mesh axis runs over, the one named last changes fastest.
Arguments:
- x: bfloat16 [4096, 8192], P('dp'), parts along dimension 0
- dy: bfloat16 [4096, 8192], P('dp'), parts along dimension 0
- gate: bfloat16 [4096, 28672], P('dp', 'tp'), parts along dimension 0
- up: bfloat16 [4096, 28672], P('dp', 'tp'), parts along dimension 0
- w_gate: bfloat16 [8192, 28672], P(None, 'tp')
- w_up: bfloat16 [8192, 28672], P(None, 'tp')
- w_down: bfloat16 [28672, 8192], P('tp')
Outputs:
- output 1: bfloat16 [4096, 8192], P('dp'), parts along dimension 0
- output 2: bfloat16 [16384, 28672], P('dp', 'tp'), parts along dimension 0
- output 3: bfloat16 [16384, 28672], P('dp', 'tp'), parts along dimension 0
- output 4: bfloat16 [57344, 8192], P(('dp', 'tp')), parts along dimension 0
There are 2 independent parts. The reference program is written for one: setup_inputs(seed, part) draws one part's arguments, and reference() takes and returns one part's arrays. A program takes and returns all parts, laid end to end along the dimension named above; an argument that names none is the same for every part.
All inputs are finite; a program needn't handle non-finite values.
Results may differ from the reference program's by a relative error of at most 0.012.
Values are sent between devices in bfloat16 or wider.
A program may use at most 2 GiB of HBM per device.

```python
import jax
import jax.numpy as jnp

ROWS = 2048
D = 8192
FF = 28672


def act(gate, up):
    return jax.nn.silu(gate) * up


def setup_inputs(seed: int = 0, part: int = 0) -> dict:
    kx, ky, ka, kb, kg, ku, kd = jax.random.split(jax.random.key(seed), 7)
    kx, ky, ka, kb = (jax.random.fold_in(k, part) for k in (kx, ky, ka, kb))
    drawn = {
        "x": jax.random.normal(kx, (ROWS, D), jnp.float32),
        "dy": jax.random.normal(ky, (ROWS, D), jnp.float32),
        "gate": jax.random.normal(ka, (ROWS, FF), jnp.float32),
        "up": jax.random.normal(kb, (ROWS, FF), jnp.float32),
        "w_gate": jax.random.normal(kg, (D, FF), jnp.float32) * D**-0.5,
        "w_up": jax.random.normal(ku, (D, FF), jnp.float32) * D**-0.5,
        "w_down": jax.random.normal(kd, (FF, D), jnp.float32) * FF**-0.5,
    }
    return {k: v.astype(jnp.bfloat16) for k, v in drawn.items()}


def reference(x, dy, gate, up, w_gate, w_up, w_down):
    hidden, back = jax.vjp(act, gate.astype(jnp.float32), up.astype(jnp.float32))
    d_hidden = jnp.dot(dy, w_down.T, preferred_element_type=jnp.float32)
    d_gate, d_up = (g.astype(jnp.bfloat16) for g in back(d_hidden))
    dx = jnp.dot(d_gate, w_gate.T, preferred_element_type=jnp.float32) + jnp.dot(d_up, w_up.T, preferred_element_type=jnp.float32)
    dw_gate = jnp.dot(x.T, d_gate, preferred_element_type=jnp.float32)
    dw_up = jnp.dot(x.T, d_up, preferred_element_type=jnp.float32)
    dw_down = jnp.dot(hidden.astype(jnp.bfloat16).T, dy, preferred_element_type=jnp.float32)
    return tuple(g.astype(jnp.bfloat16) for g in (dx, dw_gate, dw_up, dw_down))
```

```python
import jax
import jax.numpy as jnp
from jax import lax
from jax.experimental import pallas as pl
from jax.experimental.pallas import tpu as pltpu
from jax.sharding import PartitionSpec as P

BF = jnp.bfloat16
F32 = jnp.float32
VMEM_LIMIT = 67043328
CHUNKS = 4
CHIPS = 8
TILES = 7
SLOTS = 10


def nt(a, b):
    return lax.dot_general(a, b, (((1,), (1,)), ((), ())), preferred_element_type=F32)


def tn(a, b):
    return lax.dot_general(a, b, (((0,), (0,)), ((), ())), preferred_element_type=F32)


def chip_at(q):
    return q + (q // 4) * (11 - 2 * q)


def reduce_kernel(
    dy, wd, gate, up, wg, wu,
    dgo, duo, hido, piece,
    dyb, wdb, gtb, utb, dg, du, hb, wgb, wub, own, precv, psend, rrecv, rsend,
    s_dy, s_wd, s_gt, s_ut, s_og, s_ou, s_pg, s_pu, s_h, s_dg, s_du, s_fin,
    s_psend, s_precv, s_rsend, s_rrecv, c_ring, c_part,
):
    M = dyb.shape[0]
    W = wgb.shape[1] // 2
    FT = wdb.shape[1]
    i = lax.axis_index("tp")
    core = i % 2
    chip = i // 2
    y = chip // 4
    z = chip % 4
    r = z + y * (7 - 2 * z)
    sgn = 1 - 2 * core
    nxt = {"tp": 2 * chip_at((r + sgn + 8) % 8) + core}
    prv = {"tp": 2 * chip_at((r - sgn + 8) % 8) + core}
    par = {"tp": 2 * chip + 1 - core}
    MESH = pl.DeviceIdType.MESH

    def rows_own(h):
        return pl.multiple_of((2 * chip_at((r - sgn * (1 + h) + 16) % 8) + core) * W, W)

    def rows_par(h):
        return pl.multiple_of((2 * chip_at((r + sgn * (1 + h) + 16) % 8) + 1 - core) * W, W)

    def ld(src, dst, sem):
        return pltpu.make_async_copy(src, dst, sem)

    def own_w(g):
        a, k = rows_own(g % 8), g % 2
        half = pl.ds(0, W)
        return [
            ld(wg.at[pl.ds(a, W), :], wgb.at[k, half], s_og.at[k]),
            ld(wu.at[pl.ds(a, W), :], wub.at[k, half], s_ou.at[k]),
        ]

    def par_w(g):
        a, k = rows_par(g % 8), (g + 1) % 2
        half = pl.ds(W, W)
        return [
            ld(wg.at[pl.ds(a, W), :], wgb.at[k, half], s_pg.at[k]),
            ld(wu.at[pl.ds(a, W), :], wub.at[k, half], s_pu.at[k]),
        ]

    def dh_in(k):
        c, j, b = k // TILES, k % TILES, k % 2
        rows, cols = pl.ds(pl.multiple_of(c * M, M), M), pl.ds(pl.multiple_of(j * FT, FT), FT)
        return [
            ld(wd.at[cols, :], wdb.at[b], s_wd.at[b]),
            ld(gate.at[rows, cols], gtb.at[b], s_gt.at[b]),
            ld(up.at[rows, cols], utb.at[b], s_ut.at[b]),
        ]

    def dy_in(c):
        return ld(dy.at[pl.ds(pl.multiple_of(c * M, M), M), :], dyb, s_dy)

    def dh_out(k):
        c, j, b = k // TILES, k % TILES, k % 2
        rows, cols = pl.ds(pl.multiple_of(c * M, M), M), pl.ds(pl.multiple_of(j * FT, FT), FT)
        return [
            ld(hb.at[b], hido.at[rows, cols], s_h.at[b]),
            ld(dg.at[c % 2, :, cols], dgo.at[rows, cols], s_dg.at[b]),
            ld(du.at[c % 2, :, cols], duo.at[rows, cols], s_du.at[b]),
        ]

    def fin(c):
        return ld(rsend.at[3], piece.at[pl.ds(pl.multiple_of(c * M, M), M), :], s_fin)

    def ring(m):
        return pltpu.make_async_remote_copy(
            rsend.at[m % 2], rrecv.at[m % 4], s_rsend.at[m % 2], s_rrecv.at[m % 4], device_id=nxt, device_id_type=MESH
        )

    def part(g):
        return pltpu.make_async_remote_copy(
            psend.at[g % 2], precv.at[g % 4], s_psend.at[g % 2], s_precv.at[g % 4], device_id=par, device_id_type=MESH
        )

    def start(copies):
        for c in copies:
            c.start()

    def wait(copies):
        for c in copies:
            c.wait()

    def dh_tile(k):
        c, j, b = k // TILES, k % TILES, k % 2
        cols = pl.ds(pl.multiple_of(j * FT, FT), FT)
        d = nt(dyb[...], wdb[b])
        g = gtb[b].astype(F32)
        u = utb[b].astype(F32)
        sig = 1.0 / (1.0 + jnp.exp(-g))
        silu = g * sig
        hb[b] = (silu * u).astype(BF)
        du[c % 2, :, cols] = (d * silu).astype(BF)
        dg[c % 2, :, cols] = (d * u * (sig * (1.0 + g * (1.0 - sig)))).astype(BF)

    def par_tile(g):
        k, b, half = (g // 8) % 2, (g + 1) % 2, pl.ds(W, W)
        psend[g % 2] = (nt(dg[k], wgb[b, half]) + nt(du[k], wub[b, half])).astype(BF)

    def own_tile(g):
        k, b, half = (g // 8) % 2, g % 2, pl.ds(0, W)
        own[g % SLOTS] = nt(dg[k], wgb[b, half]) + nt(du[k], wub[b, half])

    def both_tiles(g):
        k, b = (g // 8) % 2, g % 2
        term = nt(dg[k], wgb[b]) + nt(du[k], wub[b])
        own[g % SLOTS] = term[:, :W]
        psend[(g + 1) % 2] = term[:, W:].astype(BF)

    def dh_ready(k):
        wait(dh_in(k))

        @pl.when(k >= 2)
        def _():
            wait(dh_out(k - 2))

    def dh_done(k):
        start(dh_out(k))

        @pl.when(k + 2 < CHUNKS * TILES)
        def _():
            start(dh_in(k + 2))

    dy_in(0).start()
    start(dh_in(0))
    start(dh_in(1))
    start(par_w(0))
    start(own_w(0))
    start(par_w(1))
    start(own_w(1))
    barrier = pltpu.get_barrier_semaphore()
    for d in (nxt, prv, par):
        pl.semaphore_signal(barrier, inc=1, device_id=d, device_id_type=MESH)
    rrecv[4] = jnp.zeros((M, W), BF)
    dy_in(0).wait()

    @pl.loop(0, TILES)
    def _(k):
        dh_ready(k)
        dh_tile(k)
        dh_done(k)

    dy_in(1).start()
    pl.semaphore_wait(barrier, 3)
    wait(par_w(0))
    par_tile(0)
    part(0).start()
    start(par_w(2))

    STEPS = CHUNKS * 8
    SENDS = CHUNKS * 7

    def combine(g):
        own[g % SLOTS] = own[g % SLOTS] + precv[(g + 4) % 4].astype(F32)

    def credit():
        pl.semaphore_signal(c_ring, inc=1, device_id=prv, device_id_type=MESH)

    @pl.loop(0, STEPS)
    def _(t):
        c, s = t // 8, t % 8
        odd = t % 2
        first = 1 - (s + 6) // 7
        later = (c + 3) // 4
        m = (1 - later) * ((t + 7) // 2 - 4) + later * (7 * c - 4 + s)
        n = (1 - later) * ((t + 5) // 2 - 4) + later * (7 * c - 6 + s + first)
        adds = (odd == 1) | (t >= 10)
        takes = adds & (s != 1)
        sends = adds & (s != 0)
        ends = adds & (s == 0)
        has_dh = (s < 7) & (c < CHUNKS - 1)
        k = TILES * (c + 1) + s
        hop = odd * ((s - 1) // 2) + (1 - odd) * ((1 - first) * (3 + s // 2) + first * 7)
        tile = (8 * (c - (1 - odd) * (1 + first)) + hop + 2 * CHUNKS * SLOTS) % SLOTS
        on = 1 - (1 - odd) * ((41 - t) // 32)
        got = on * (1 - odd * ((8 - s) // 7))
        src = got * ((n + 8) % 4) + (1 - got) * 4
        dst = on * ((1 - first) * ((m + 8) % 2) + first * 3) + (1 - on) * 2

        wait(own_w(t))

        @pl.when(t + 1 < STEPS)
        def _():
            wait(par_w(t + 1))

        @pl.when((s == 0) & (c < CHUNKS - 1))
        def _():
            dy_in(c + 1).wait()

        @pl.when(has_dh)
        def _():
            dh_ready(k)

        @pl.when(t >= 1)
        def _():
            part(t - 1).wait_recv()
            part(t - 1).wait_send()

        @pl.when(takes)
        def _():
            ring(n).wait_recv()

        @pl.when(sends & (m >= 2))
        def _():
            ring(m - 2).wait_send()

        @pl.when(ends & (c >= 3))
        def _():
            fin(c - 3).wait()

        def add():
            combine(t - 1 + SLOTS * 4)
            rsend[dst] = (own[tile] + rrecv[src].astype(F32)).astype(BF)

        def send():
            @pl.when(sends & (m >= 4))
            def _():
                pl.semaphore_wait(c_ring, 1)

            @pl.when(sends)
            def _():
                ring(m).start()

            @pl.when(ends)
            def _():
                fin(c - 2).start()

            @pl.when(takes & (n < SENDS - 4))
            def _():
                credit()

        @pl.when(has_dh)
        def _():
            dh_tile(k)

            @pl.when(t >= 0)
            def _():
                both_tiles(t)

            add()
            send()
            dh_done(k)

        @pl.when(jnp.logical_not(has_dh))
        def _():
            add()
            send()
            own_tile(t)

            @pl.when(t + 1 < STEPS)
            def _():
                par_tile(t + 1)

        @pl.when(t + 1 < STEPS)
        def _():
            @pl.when(t >= 2)
            def _():
                pl.semaphore_wait(c_part, 1)

            part(t + 1).start()

        @pl.when(t < STEPS - 3)
        def _():
            pl.semaphore_signal(c_part, inc=1, device_id=par, device_id_type=MESH)

        @pl.when((s == 6) & (c < CHUNKS - 2))
        def _():
            dy_in(c + 2).start()

        @pl.when(t + 2 < STEPS)
        def _():
            start(own_w(t + 2))

        @pl.when(t + 3 < STEPS)
        def _():
            start(par_w(t + 3))

    part(STEPS - 1).wait_recv()
    part(STEPS - 1).wait_send()
    combine(STEPS - 1)
    n = SENDS - 5
    for tile in (STEPS - 9, STEPS - 4, STEPS - 3, STEPS - 2, STEPS - 1):
        ring(n).wait_recv()
        last = tile % 8 == 7
        if last:
            fin(0).wait()
            dst = 3
        else:
            m = n + 1
            ring(m - 2).wait_send()
            dst = m % 2
        rsend[dst] = (own[tile % SLOTS] + rrecv[n % 4].astype(F32)).astype(BF)
        if last:
            fin(tile // 8).start()
        else:
            pl.semaphore_wait(c_ring, 1)
            ring(m).start()
        if n < SENDS - 4:
            credit()
        n += 1
    ring(SENDS - 2).wait_send()
    ring(SENDS - 1).wait_send()
    fin(0).wait()
    wait(dh_out(CHUNKS * TILES - 2))
    wait(dh_out(CHUNKS * TILES - 1))


def reduce_call(dy, wd, gate, up, wg, wu):
    T, D = dy.shape
    F = gate.shape[1]
    M, W, FT = T // CHUNKS, D // (2 * CHIPS), F // TILES
    hbm = pl.BlockSpec(memory_space=pltpu.HBM)
    dma, reg = pltpu.SemaphoreType.DMA, pltpu.SemaphoreType.REGULAR
    v = pltpu.VMEM
    return pl.pallas_call(
        reduce_kernel,
        in_specs=[hbm] * 6,
        out_specs=[hbm] * 4,
        out_shape=[jax.ShapeDtypeStruct((T, F), BF)] * 3 + [jax.ShapeDtypeStruct((T, W), BF)],
        scratch_shapes=[
            v((M, D), BF), v((2, FT, D), BF), v((2, M, FT), BF), v((2, M, FT), BF),
            v((2, M, F), BF), v((2, M, F), BF), v((2, M, FT), BF),
            v((2, 2 * W, F), BF), v((2, 2 * W, F), BF),
            v((SLOTS, M, W), F32), v((4, M, W), BF), v((2, M, W), BF), v((5, M, W), BF), v((4, M, W), BF),
            dma(()), *[dma((2,))] * 10, dma(()),
            dma((2,)), dma((4,)), dma((2,)), dma((4,)), reg, reg,
        ],
        compiler_params=pltpu.CompilerParams(collective_id=0, has_side_effects=True, vmem_limit_bytes=VMEM_LIMIT),
        name="dx_reduce",
    )(dy, wd, gate, up, wg, wu)


def gate_up_grads(x, dg, du, bm):
    T, D = x.shape
    F = dg.shape[1]

    def body(x_ref, dg_ref, du_ref, og, ou):
        og[...] = tn(x_ref[...], dg_ref[...]).astype(BF)
        ou[...] = tn(x_ref[...], du_ref[...]).astype(BF)

    one = pl.BlockSpec((T, F), lambda i: (0, 0), pipeline_mode=pl.Buffered(1))
    return pl.pallas_call(
        body,
        grid=(D // bm,),
        in_specs=[pl.BlockSpec((T, bm), lambda i: (0, i)), one, one],
        out_specs=[pl.BlockSpec((bm, F), lambda i: (i, 0))] * 2,
        out_shape=[jax.ShapeDtypeStruct((D, F), BF)] * 2,
        compiler_params=pltpu.CompilerParams(vmem_limit_bytes=VMEM_LIMIT),
        cost_estimate=pl.CostEstimate(flops=4 * T * D * F, bytes_accessed=2 * (T * D + 2 * T * F + 2 * D * F), transcendentals=0),
        name="dw_gate_up",
    )(x, dg, du)


def down_grad(hid, dy, bn, lo, hi, moved=(), prev=()):
    T, D = dy.shape
    F = hid.shape[1]
    steps = hi - lo
    mb = T // steps

    def body(h_ref, dy_ref, *refs):
        if moved:
            refs[-1][...] = refs[0][...]
        o_ref = refs[-2] if moved else refs[-1]
        o_ref[...] = tn(h_ref[...], dy_ref[...]).astype(BF)

    rows = [pl.BlockSpec((mb, D), lambda i: (i, 0))] if moved else []
    return pl.pallas_call(
        body,
        grid=(steps,),
        in_specs=[
            pl.BlockSpec((T, F), lambda i: (0, 0), pipeline_mode=pl.Buffered(1)),
            pl.BlockSpec((T, bn), lambda i: (0, lo + i)),
            *rows,
            *[pl.BlockSpec(memory_space=pl.ANY)] * len(prev),
        ],
        out_specs=[pl.BlockSpec((F, bn), lambda i: (0, lo + i)), *rows],
        out_shape=[jax.ShapeDtypeStruct((F, D), BF), *[jax.ShapeDtypeStruct((T, D), BF)] * len(moved)],
        input_output_aliases={2 + len(moved): 0} if prev else {},
        compiler_params=pltpu.CompilerParams(vmem_limit_bytes=VMEM_LIMIT),
        cost_estimate=pl.CostEstimate(
            flops=2 * T * F * bn * steps,
            bytes_accessed=2 * (T * F + (T + F) * bn * steps + 2 * T * D * len(moved)),
            transcendentals=0,
        ),
        name="dw_down",
    )(hid, dy, *moved, *prev)


def solution(mesh):
    def step(x, dy, gate, up, w_gate, w_up, w_down):
        D = x.shape[1]
        dg, du, hid, piece = reduce_call(dy, w_down, gate, up, w_gate, w_up)
        gathered = lax.all_gather(piece, "tp", axis=1, tiled=True)
        dw_gate, dw_up = gate_up_grads(x, dg, du, D // 16)
        bn = D // 16
        first = down_grad(hid, dy, bn, 0, 8)
        dw_down, dx = down_grad(hid, dy, bn, 8, 16, (gathered,), first)
        return dx, dw_gate, dw_up, dw_down

    tokens, columns, rows = P("dp", None), P(None, "tp"), P("tp", None)
    return jax.shard_map(
        step,
        mesh=mesh,
        in_specs=(tokens, tokens, P("dp", "tp"), P("dp", "tp"), columns, columns, rows),
        out_specs=(tokens, P("dp", "tp"), P("dp", "tp"), P(("dp", "tp"), None)),
        check_vma=False,
    )
```

```python
import jax
import jax.numpy as jnp
from jax import lax
from jax.experimental import pallas as pl
from jax.experimental.pallas import tpu as pltpu
from jax.sharding import PartitionSpec as P

BF = jnp.bfloat16
F32 = jnp.float32
VMEM_LIMIT = 67043328
CHUNKS = 4
CHIPS = 8
TILES = 7
STEPS = CHUNKS * CHIPS
SENDS = CHUNKS * (CHIPS - 1)


def nt(a, b):
    return lax.dot_general(a, b, (((1,), (1,)), ((), ())), preferred_element_type=F32)


def tn(a, b):
    return lax.dot_general(a, b, (((0,), (0,)), ((), ())), preferred_element_type=F32)


def chip_at(q):
    return q + (q // 4) * (11 - 2 * q)


def reduce_kernel(
    dy, wd, gate, up, wg, wu,
    dguo, hido, piece,
    dyb, wdb, gtb, utb, dg, du, dgn, dun, hb, wgb, wub, own, precv, psend, rrecv, rsend,
    s_dy, s_wd, s_gt, s_ut, s_og, s_ou, s_pg, s_pu, s_h, s_dg, s_du, s_fin,
    s_psend, s_precv, s_rsend, s_rrecv, c_ring, c_part,
):
    M, D = dyb.shape[1:]
    W = wgb.shape[1] // 2
    F, FT = dg.shape[1], wdb.shape[1]
    H = M // 2
    i = lax.axis_index("tp")
    core = i % 2
    chip = i // 2
    y = chip // 4
    z = chip % 4
    r = z + y * (7 - 2 * z)
    sgn = 1 - 2 * core
    nxt = {"tp": 2 * chip_at((r + sgn + 8) % 8) + core}
    prv = {"tp": 2 * chip_at((r - sgn + 8) % 8) + core}
    par = {"tp": 2 * chip + 1 - core}
    MESH = pl.DeviceIdType.MESH

    def rows_own(h):
        return pl.multiple_of((2 * chip_at((r - sgn * (1 + h) + 16) % 8) + core) * W, W)

    def rows_par(h):
        return pl.multiple_of((2 * chip_at((r + sgn * (1 + h) + 16) % 8) + 1 - core) * W, W)

    ld = pltpu.make_async_copy

    def own_w(g):
        a, k, half = rows_own(g % 8), g % 2, pl.ds(0, W)
        return [
            ld(wg.at[pl.ds(a, W), :], wgb.at[k, half], s_og.at[k]),
            ld(wu.at[pl.ds(a, W), :], wub.at[k, half], s_ou.at[k]),
        ]

    def par_w(g):
        a, k, half = rows_par(g % 8), (g + 1) % 2, pl.ds(W, W)
        return [
            ld(wg.at[pl.ds(a, W), :], wgb.at[k, half], s_pg.at[k]),
            ld(wu.at[pl.ds(a, W), :], wub.at[k, half], s_pu.at[k]),
        ]

    def dh_place(k):
        c, j = k // TILES, k % TILES
        return pl.ds(pl.multiple_of(c * M, M), M), pl.ds(pl.multiple_of(j * FT, FT), FT)

    def dh_in(k):
        b = k % 2
        rows, cols = dh_place(k)
        return [
            ld(wd.at[cols, :], wdb.at[b], s_wd.at[b]),
            ld(gate.at[rows, cols], gtb.at[b], s_gt.at[b]),
            ld(up.at[rows, cols], utb.at[b], s_ut.at[b]),
        ]

    def dy_in(c, p):
        n = M // 4
        return ld(dy.at[pl.ds(pl.multiple_of(c * M + p * n, n), n), :], dyb.at[c % 2, pl.ds(p * n, n)], s_dy.at[p])

    def dh_out(k, dg, du):
        b = k % 2
        rows, cols = dh_place(k)
        return [
            ld(hb.at[b], hido.at[rows, cols], s_h.at[b]),
            ld(dg.at[:, cols], dguo.at[rows, cols], s_dg.at[b]),
            ld(du.at[:, cols], dguo.at[rows, pl.ds(pl.multiple_of(F + k % TILES * FT, FT), FT)], s_du.at[b]),
        ]

    def fin(e, c):
        return ld(rsend.at[e, 2], piece.at[pl.ds(pl.multiple_of(c * M + e * H, H), H), :], s_fin.at[e])

    def ring(e, m):
        return pltpu.make_async_remote_copy(
            rsend.at[e, m % 2], rrecv.at[e, m % 3], s_rsend.at[e, m % 2], s_rrecv.at[e, m % 3], device_id=nxt, device_id_type=MESH
        )

    def part(g):
        return pltpu.make_async_remote_copy(
            psend.at[g % 2], precv.at[g % 4], s_psend.at[g % 2], s_precv.at[g % 4], device_id=par, device_id_type=MESH
        )

    def start(copies):
        for c in copies:
            c.start()

    def wait(copies):
        for c in copies:
            c.wait()

    def dh_tile(k, dg, du):
        b, cols = k % 2, dh_place(k)[1]
        d = nt(dyb[(k // TILES) % 2], wdb[b])
        g = gtb[b].astype(F32)
        u = utb[b].astype(F32)
        sig = lax.logistic(g)
        silu = g * sig
        hb[b] = (silu * u).astype(BF)
        du[:, cols] = (d * silu).astype(BF)
        dg[:, cols] = (d * u * (sig * (1.0 + g * (1.0 - sig)))).astype(BF)

    def own_tile(g):
        b, half = g % 2, pl.ds(0, W)
        own[g % 2] = nt(dg[...], wgb[b, half]) + nt(du[...], wub[b, half])

    def par_tile(g, dg, du):
        b, half = (g + 1) % 2, pl.ds(W, W)
        psend[g % 2] = (nt(dg[...], wgb[b, half]) + nt(du[...], wub[b, half])).astype(BF)

    def add(e, g, src, dst):
        rows = pl.ds(e * H, H)
        total = own[g % 2, rows] + precv[(g + 4) % 4, rows].astype(F32) + rrecv[e, src].astype(F32)
        rsend[e, dst] = total.astype(BF)

    def dh_ready(k):
        wait(dh_in(k))

        @pl.when(k >= 2)
        def _():
            wait(dh_out(k - 2, dg, du))

    def dh_done(k, dg, du):
        start(dh_out(k, dg, du))

        @pl.when(k + 2 < CHUNKS * TILES)
        def _():
            start(dh_in(k + 2))

    start(dh_in(0))
    for p in range(4):
        dy_in(0, p).start()
    start(dh_in(1))
    start(par_w(0))
    start(own_w(0))
    start(par_w(1))
    start(own_w(1))
    barrier = pltpu.get_barrier_semaphore()
    for d in (nxt, prv, par):
        pl.semaphore_signal(barrier, inc=1, device_id=d, device_id_type=MESH)
    for e in range(2):
        rrecv[e, 3] = jnp.zeros((H, W), BF)

    @pl.loop(0, TILES)
    def _(k):
        @pl.when(k == 0)
        def _():
            for p in range(4):
                dy_in(0, p).wait()

        dh_ready(k)
        dh_tile(k, dg, du)
        dh_done(k, dg, du)

        @pl.when(k < 4)
        def _():
            dy_in(1, k).start()

    wait(par_w(0))
    par_tile(0, dg, du)
    pl.semaphore_wait(barrier, 3)
    part(0).start()
    start(par_w(2))

    @pl.loop(0, STEPS)
    def _(t):
        c, s = t // 8, t % 8
        has_dh = (s < 7) & (c < CHUNKS - 1)
        k = TILES * (c + 1) + s
        g = t - 1
        h = (g + 8) % 8
        m = 7 * ((g + 8) // 8 - 1) + h
        adds = t >= 1
        takes = adds & (h >= 1)
        sends = adds & (h <= 6)
        ends = adds & (h == 7)
        last = (h + 1) // 8
        got = (h + 7) // 8 * (1 - (STEPS - t) // STEPS)
        src = got * ((m + 2) % 3) + (1 - got) * 3
        dst = (1 - last) * (m % 2) + last * 2

        wait(own_w(t))

        @pl.when(t + 1 < STEPS)
        def _():
            wait(par_w(t + 1))

        @pl.when((s == 0) & (c < CHUNKS - 1))
        def _():
            for p in range(4):
                dy_in(c + 1, p).wait()

        @pl.when(has_dh)
        def _():
            dh_ready(k)

        @pl.when(adds)
        def _():
            part(g).wait_recv()
            part(g).wait_send()

        @pl.when(sends & (m >= 2))
        def _():
            for e in range(2):
                ring(e, m - 2).wait_send()

        @pl.when(sends & (m >= 3))
        def _():
            for e in range(2):
                pl.semaphore_wait(c_ring.at[e], 1)

        @pl.when(ends & (t >= 16))
        def _():
            for e in range(2):
                fin(e, c - 2).wait()

        def pass_on(e):
            @pl.when(takes)
            def _():
                ring(e, m - 1).wait_recv()

            add(e, g, src, dst)

            @pl.when(sends)
            def _():
                ring(e, m).start()

        pass_on(0)

        @pl.when(has_dh)
        def _():
            dh_tile(k, dgn, dun)

        @pl.when(jnp.logical_not(has_dh))
        def _():
            own_tile(t)

        pass_on(1)

        @pl.when(has_dh)
        def _():
            own_tile(t)
            par_tile(t + 1, dg, du)
            dh_done(k, dgn, dun)

        @pl.when((s < 7) & (c == CHUNKS - 1))
        def _():
            par_tile(t + 1, dg, du)

        @pl.when((s == 7) & (c < CHUNKS - 1))
        def _():
            par_tile(t + 1, dgn, dun)
            dg[...] = dgn[...]
            du[...] = dun[...]

        @pl.when(ends)
        def _():
            for e in range(2):
                fin(e, c - 1).start()

        @pl.when(t + 1 < STEPS)
        def _():
            @pl.when(t >= 2)
            def _():
                pl.semaphore_wait(c_part, 1)

            part(t + 1).start()

        @pl.when(takes & (m - 1 < SENDS - 3))
        def _():
            for e in range(2):
                pl.semaphore_signal(c_ring.at[e], inc=1, device_id=prv, device_id_type=MESH)

        @pl.when(t < STEPS - 3)
        def _():
            pl.semaphore_signal(c_part, inc=1, device_id=par, device_id_type=MESH)

        @pl.when((s < 4) & (c < CHUNKS - 2))
        def _():
            dy_in(c + 2, s).start()

        @pl.when(t + 2 < STEPS)
        def _():
            start(own_w(t + 2))

        @pl.when(t + 3 < STEPS)
        def _():
            start(par_w(t + 3))

    part(STEPS - 1).wait_recv()
    part(STEPS - 1).wait_send()
    for e in range(2):
        fin(e, CHUNKS - 2).wait()
        ring(e, SENDS - 1).wait_recv()
        add(e, STEPS - 1, (SENDS - 1) % 3, 2)
        fin(e, CHUNKS - 1).start()
    for e in range(2):
        ring(e, SENDS - 2).wait_send()
        ring(e, SENDS - 1).wait_send()
        fin(e, CHUNKS - 1).wait()
    wait(dh_out(CHUNKS * TILES - 2, dgn, dun))
    wait(dh_out(CHUNKS * TILES - 1, dgn, dun))


def reduce_call(dy, wd, gate, up, wg, wu):
    T, D = dy.shape
    F = gate.shape[1]
    M, W, FT = T // CHUNKS, D // (2 * CHIPS), F // TILES
    hbm = pl.BlockSpec(memory_space=pltpu.HBM)
    dma, reg = pltpu.SemaphoreType.DMA, pltpu.SemaphoreType.REGULAR
    v = pltpu.VMEM
    return pl.pallas_call(
        reduce_kernel,
        in_specs=[hbm] * 6,
        out_specs=[hbm] * 3,
        out_shape=[jax.ShapeDtypeStruct((T, n), BF) for n in (2 * F, F, W)],
        scratch_shapes=[
            v((2, M, D), BF), v((2, FT, D), BF), v((2, M, FT), BF), v((2, M, FT), BF),
            v((M, F), BF), v((M, F), BF), v((M, F), BF), v((M, F), BF), v((2, M, FT), BF), v((2, 2 * W, F), BF), v((2, 2 * W, F), BF),
            v((2, M, W), F32), v((4, M, W), BF), v((2, M, W), BF), v((2, 4, M // 2, W), BF), v((2, 3, M // 2, W), BF),
            dma((4,)), *[dma((2,))] * 11,
            dma((2,)), dma((4,)), dma((2, 2)), dma((2, 3)), reg((2,)), reg,
        ],
        compiler_params=pltpu.CompilerParams(collective_id=0, has_side_effects=True, vmem_limit_bytes=VMEM_LIMIT),
        name="dx_reduce",
    )(dy, wd, gate, up, wg, wu)


def gate_up_grads(x, dgu, bm):
    T, D = x.shape
    F = dgu.shape[1] // 2

    def body(x_ref, d_ref, og, ou):
        both = tn(x_ref[...], d_ref[...])
        og[...] = both[:, :F].astype(BF)
        ou[...] = both[:, F:].astype(BF)

    return pl.pallas_call(
        body,
        grid=(D // bm,),
        in_specs=[
            pl.BlockSpec((T, bm), lambda i: (0, i)),
            pl.BlockSpec((T, 2 * F), lambda i: (0, 0), pipeline_mode=pl.Buffered(1)),
        ],
        out_specs=[pl.BlockSpec((bm, F), lambda i: (i, 0))] * 2,
        out_shape=[jax.ShapeDtypeStruct((D, F), BF)] * 2,
        compiler_params=pltpu.CompilerParams(vmem_limit_bytes=VMEM_LIMIT),
        cost_estimate=pl.CostEstimate(flops=4 * T * D * F, bytes_accessed=2 * (T * D + 2 * T * F + 2 * D * F), transcendentals=0),
        name="dw_gate_up",
    )(x, dgu)


def down_grad(hid, dy, bn, lo, hi, moved=(), prev=()):
    T, D = dy.shape
    F = hid.shape[1]
    steps = hi - lo
    mb = T // steps

    def body(h_ref, dy_ref, *refs):
        if moved:
            refs[-1][...] = refs[0][...]
        o_ref = refs[-2] if moved else refs[-1]
        o_ref[...] = tn(h_ref[...], dy_ref[...]).astype(BF)

    rows = [pl.BlockSpec((mb, D), lambda i: (i, 0))] if moved else []
    return pl.pallas_call(
        body,
        grid=(steps,),
        in_specs=[
            pl.BlockSpec((T, F), lambda i: (0, 0), pipeline_mode=pl.Buffered(1)),
            pl.BlockSpec((T, bn), lambda i: (0, lo + i)),
            *rows,
            *[pl.BlockSpec(memory_space=pl.ANY)] * len(prev),
        ],
        out_specs=[pl.BlockSpec((F, bn), lambda i: (0, lo + i)), *rows],
        out_shape=[jax.ShapeDtypeStruct((F, D), BF), *[jax.ShapeDtypeStruct((T, D), BF)] * len(moved)],
        input_output_aliases={2 + len(moved): 0} if prev else {},
        compiler_params=pltpu.CompilerParams(vmem_limit_bytes=VMEM_LIMIT),
        cost_estimate=pl.CostEstimate(
            flops=2 * T * F * bn * steps,
            bytes_accessed=2 * (T * F + (T + F) * bn * steps + 2 * T * D * len(moved)),
            transcendentals=0,
        ),
        name="dw_down",
    )(hid, dy, *moved, *prev)


def solution(mesh):
    def step(x, dy, gate, up, w_gate, w_up, w_down):
        D = x.shape[1]
        dgu, hid, piece = reduce_call(dy, w_down, gate, up, w_gate, w_up)
        gathered = lax.all_gather(piece, "tp", axis=1, tiled=True)
        dw_gate, dw_up = gate_up_grads(x, dgu, D // 16)
        bn = D // 16
        first = down_grad(hid, dy, bn, 0, 8)
        dw_down, dx = down_grad(hid, dy, bn, 8, 16, (gathered,), first)
        return dx, dw_gate, dw_up, dw_down

    tokens, columns, rows = P("dp", None), P(None, "tp"), P("tp", None)
    return jax.shard_map(
        step,
        mesh=mesh,
        in_specs=(tokens, tokens, P("dp", "tp"), P("dp", "tp"), columns, columns, rows),
        out_specs=(tokens, P("dp", "tp"), P("dp", "tp"), P(("dp", "tp"), None)),
        check_vma=False,
    )
```

```python
import jax
import jax.numpy as jnp
from jax import lax
from jax.experimental import pallas as pl
from jax.experimental.pallas import tpu as pltpu
from jax.sharding import PartitionSpec as P

BF = jnp.bfloat16
F32 = jnp.float32
VMEM_LIMIT = 67043328
CHUNKS = 4
CHIPS = 8
TILES = 7
STEPS = CHUNKS * CHIPS
SENDS = CHUNKS * (CHIPS - 1)
EXTRA = 8


def nt(a, b):
    return lax.dot_general(a, b, (((1,), (1,)), ((), ())), preferred_element_type=F32)


def tn(a, b):
    return lax.dot_general(a, b, (((0,), (0,)), ((), ())), preferred_element_type=F32)


def chip_at(q):
    return q + (q // 4) * (11 - 2 * q)


def reduce_kernel(
    dy, wd, gate, up, wg, wu,
    dguo, hido, piece, extra,
    dyb, wdb, gtb, utb, dg, du, dgn, dun, hb, wgb, wub, own, precv, psend, rrecv, rsend, fout,
    s_dy, s_fd, s_fo, s_wd, s_gt, s_ut, s_og, s_ou, s_pg, s_pu, s_h, s_dg, s_du, s_fin,
    s_psend, s_precv, s_rsend, s_rrecv, c_ring, c_part,
):
    M, D = dyb.shape[1:]
    W = wgb.shape[1] // 2
    F, FT = dg.shape[1], wdb.shape[1]
    H = M // 2
    i = lax.axis_index("tp")
    core = i % 2
    chip = i // 2
    y = chip // 4
    z = chip % 4
    r = z + y * (7 - 2 * z)
    sgn = 1 - 2 * core
    nxt = {"tp": 2 * chip_at((r + sgn + 8) % 8) + core}
    prv = {"tp": 2 * chip_at((r - sgn + 8) % 8) + core}
    par = {"tp": 2 * chip + 1 - core}
    MESH = pl.DeviceIdType.MESH

    def rows_own(h):
        return pl.multiple_of((2 * chip_at((r - sgn * (1 + h) + 16) % 8) + core) * W, W)

    def rows_par(h):
        return pl.multiple_of((2 * chip_at((r + sgn * (1 + h) + 16) % 8) + 1 - core) * W, W)

    ld = pltpu.make_async_copy

    def own_w(g):
        a, k, half = rows_own(g % 8), g % 2, pl.ds(0, W)
        return [
            ld(wg.at[pl.ds(a, W), :], wgb.at[k, half], s_og.at[k]),
            ld(wu.at[pl.ds(a, W), :], wub.at[k, half], s_ou.at[k]),
        ]

    def par_w(g):
        a, k, half = rows_par(g % 8), (g + 1) % 2, pl.ds(W, W)
        return [
            ld(wg.at[pl.ds(a, W), :], wgb.at[k, half], s_pg.at[k]),
            ld(wu.at[pl.ds(a, W), :], wub.at[k, half], s_pu.at[k]),
        ]

    def dh_place(k):
        c, j = k // TILES, k % TILES
        return pl.ds(pl.multiple_of(c * M, M), M), pl.ds(pl.multiple_of(j * FT, FT), FT)

    def dh_in(k):
        b = k % 2
        rows, cols = dh_place(k)
        return [
            ld(wd.at[cols, :], wdb.at[b], s_wd.at[b]),
            ld(gate.at[rows, cols], gtb.at[b], s_gt.at[b]),
            ld(up.at[rows, cols], utb.at[b], s_ut.at[b]),
        ]

    def dy_in(c, p):
        n = M // 4
        return ld(dy.at[pl.ds(pl.multiple_of(c * M + p * n, n), n), :], dyb.at[c % 2, pl.ds(p * n, n)], s_dy.at[p])

    def dh_out(k, dg, du):
        b = k % 2
        rows, cols = dh_place(k)
        return [
            ld(hb.at[b], hido.at[rows, cols], s_h.at[b]),
            ld(dg.at[:, cols], dguo.at[rows, cols], s_dg.at[b]),
            ld(du.at[:, cols], dguo.at[rows, pl.ds(pl.multiple_of(F + k % TILES * FT, FT), FT)], s_du.at[b]),
        ]

    def extra_in(c):
        n = extra.shape[1]
        return [
            ld(hido.at[pl.ds(c * M, M), :], dyb.at[0, :, pl.ds(c * F, F)], s_dy.at[c]),
            ld(dy.at[pl.ds(c * M, M), pl.ds(0, n)], dyb.at[1, :, pl.ds(c * n, n)], s_fd.at[c]),
        ]

    def extra_out(u):
        rows, cols = pl.ds(pl.multiple_of(u % 2 * (F // 2), F // 2), F // 2), pl.ds(pl.multiple_of(u // 2 * FT, FT), FT)
        return ld(fout.at[u % 2], extra.at[rows, cols], s_fo.at[u % 2])

    def fin(e, c):
        return ld(rsend.at[e, 2], piece.at[pl.ds(pl.multiple_of(c * M + e * H, H), H), :], s_fin.at[e])

    def ring(e, m):
        return pltpu.make_async_remote_copy(
            rsend.at[e, m % 2], rrecv.at[e, m % 3], s_rsend.at[e, m % 2], s_rrecv.at[e, m % 3], device_id=nxt, device_id_type=MESH
        )

    def part(g):
        return pltpu.make_async_remote_copy(
            psend.at[g % 2], precv.at[g % 4], s_psend.at[g % 2], s_precv.at[g % 4], device_id=par, device_id_type=MESH
        )

    def start(copies):
        for c in copies:
            c.start()

    def wait(copies):
        for c in copies:
            c.wait()

    def dh_tile(k, dg, du):
        b, cols = k % 2, dh_place(k)[1]
        d = nt(dyb[(k // TILES) % 2], wdb[b])
        g = gtb[b].astype(F32)
        u = utb[b].astype(F32)
        sig = lax.logistic(g)
        silu = g * sig
        hb[b] = (silu * u).astype(BF)
        du[:, cols] = (d * silu).astype(BF)
        dg[:, cols] = (d * u * (sig * (1.0 + g * (1.0 - sig)))).astype(BF)

    def own_tile(g):
        b, half = g % 2, pl.ds(0, W)
        own[g % 2] = nt(dg[...], wgb[b, half]) + nt(du[...], wub[b, half])

    def par_tile(g, dg, du):
        b, half = (g + 1) % 2, pl.ds(W, W)
        psend[g % 2] = (nt(dg[...], wgb[b, half]) + nt(du[...], wub[b, half])).astype(BF)

    def add(e, g, src, dst):
        rows = pl.ds(e * H, H)
        total = own[g % 2, rows] + precv[(g + 4) % 4, rows].astype(F32) + rrecv[e, src].astype(F32)
        rsend[e, dst] = total.astype(BF)

    def extra_piece(u):
        n, half = extra.shape[1], F // 2
        total = None
        for c in range(CHUNKS):
            h = dyb[0, :, pl.ds(pl.multiple_of(c * F + u % 2 * half, half), half)]
            d = dyb[1, :, pl.ds(pl.multiple_of(c * n + u // 2 * FT, FT), FT)]
            term = tn(h, d)
            total = term if c == 0 else total + term
        fout[u % 2] = total.astype(BF)

    def dh_ready(k):
        wait(dh_in(k))

        @pl.when(k >= 2)
        def _():
            wait(dh_out(k - 2, dg, du))

    def dh_done(k, dg, du):
        start(dh_out(k, dg, du))

        @pl.when(k + 2 < CHUNKS * TILES)
        def _():
            start(dh_in(k + 2))

    start(dh_in(0))
    for p in range(4):
        dy_in(0, p).start()
    start(dh_in(1))
    start(par_w(0))
    start(own_w(0))
    start(par_w(1))
    start(own_w(1))
    barrier = pltpu.get_barrier_semaphore()
    for d in (nxt, prv, par):
        pl.semaphore_signal(barrier, inc=1, device_id=d, device_id_type=MESH)
    for e in range(2):
        rrecv[e, 3] = jnp.zeros((H, W), BF)

    @pl.loop(0, TILES)
    def _(k):
        @pl.when(k == 0)
        def _():
            for p in range(4):
                dy_in(0, p).wait()

        dh_ready(k)
        dh_tile(k, dg, du)
        dh_done(k, dg, du)

        @pl.when(k < 4)
        def _():
            dy_in(1, k).start()

    wait(par_w(0))
    par_tile(0, dg, du)
    pl.semaphore_wait(barrier, 3)
    part(0).start()
    start(par_w(2))

    @pl.loop(0, STEPS)
    def _(t):
        c, s = t // 8, t % 8
        has_dh = (s < 7) & (c < CHUNKS - 1)
        k = TILES * (c + 1) + s
        g = t - 1
        h = (g + 8) % 8
        m = 7 * ((g + 8) // 8 - 1) + h
        adds = t >= 1
        takes = adds & (h >= 1)
        sends = adds & (h <= 6)
        ends = adds & (h == 7)
        last = (h + 1) // 8
        got = (h + 7) // 8 * (1 - (STEPS - t) // STEPS)
        src = got * ((m + 2) % 3) + (1 - got) * 3
        dst = (1 - last) * (m % 2) + last * 2

        wait(own_w(t))

        @pl.when(t + 1 < STEPS)
        def _():
            wait(par_w(t + 1))

        @pl.when((s == 0) & (c < CHUNKS - 1))
        def _():
            for p in range(4):
                dy_in(c + 1, p).wait()

        @pl.when(has_dh)
        def _():
            dh_ready(k)

        @pl.when(adds)
        def _():
            part(g).wait_recv()
            part(g).wait_send()

        @pl.when(sends & (m >= 2))
        def _():
            for e in range(2):
                ring(e, m - 2).wait_send()

        @pl.when(sends & (m >= 3))
        def _():
            for e in range(2):
                pl.semaphore_wait(c_ring.at[e], 1)

        @pl.when(ends & (t >= 16))
        def _():
            for e in range(2):
                fin(e, c - 2).wait()

        def pass_on(e):
            @pl.when(takes)
            def _():
                ring(e, m - 1).wait_recv()

            add(e, g, src, dst)

            @pl.when(sends)
            def _():
                ring(e, m).start()

        pass_on(0)

        @pl.when(has_dh)
        def _():
            dh_tile(k, dgn, dun)

        @pl.when(jnp.logical_not(has_dh))
        def _():
            own_tile(t)

        pass_on(1)

        @pl.when(has_dh)
        def _():
            own_tile(t)
            par_tile(t + 1, dg, du)
            dh_done(k, dgn, dun)

        @pl.when((s < 7) & (c == CHUNKS - 1))
        def _():
            par_tile(t + 1, dg, du)

        @pl.when((s == 7) & (c < CHUNKS - 1))
        def _():
            par_tile(t + 1, dgn, dun)
            dg[...] = dgn[...]
            du[...] = dun[...]

        @pl.when(t == 8 * (CHUNKS - 1))
        def _():
            for b in range(CHUNKS):
                wait(extra_in(b))

        @pl.when(t > 8 * (CHUNKS - 1))
        def _():
            u = t - 8 * (CHUNKS - 1) - 1

            @pl.when(u >= 2)
            def _():
                extra_out(u - 2).wait()

            extra_piece(u)
            extra_out(u).start()

        @pl.when(ends)
        def _():
            for e in range(2):
                fin(e, c - 1).start()

        @pl.when(t + 1 < STEPS)
        def _():
            @pl.when(t >= 2)
            def _():
                pl.semaphore_wait(c_part, 1)

            part(t + 1).start()

        @pl.when(takes & (m - 1 < SENDS - 3))
        def _():
            for e in range(2):
                pl.semaphore_signal(c_ring.at[e], inc=1, device_id=prv, device_id_type=MESH)

        @pl.when(t < STEPS - 3)
        def _():
            pl.semaphore_signal(c_part, inc=1, device_id=par, device_id_type=MESH)

        @pl.when((s < 4) & (c < CHUNKS - 2))
        def _():
            dy_in(c + 2, s).start()

        @pl.when(t + 2 < STEPS)
        def _():
            start(own_w(t + 2))

        @pl.when(t + 3 < STEPS)
        def _():
            start(par_w(t + 3))

        @pl.when(t == 8 * (CHUNKS - 1) - 1)
        def _():
            for k in (CHUNKS * TILES - 2, CHUNKS * TILES - 1):
                wait(dh_out(k, dgn, dun))
            for b in range(CHUNKS):
                start(extra_in(b))

    part(STEPS - 1).wait_recv()
    part(STEPS - 1).wait_send()
    for e in range(2):
        fin(e, CHUNKS - 2).wait()
        if e == 1:
            extra_out(EXTRA - 3).wait()
            extra_piece(EXTRA - 1)
            extra_out(EXTRA - 1).start()
        ring(e, SENDS - 1).wait_recv()
        add(e, STEPS - 1, (SENDS - 1) % 3, 2)
        fin(e, CHUNKS - 1).start()
    for e in range(2):
        ring(e, SENDS - 2).wait_send()
        ring(e, SENDS - 1).wait_send()
        fin(e, CHUNKS - 1).wait()
    extra_out(EXTRA - 2).wait()
    extra_out(EXTRA - 1).wait()


def reduce_call(dy, wd, gate, up, wg, wu):
    T, D = dy.shape
    F = gate.shape[1]
    M, W, FT = T // CHUNKS, D // (2 * CHIPS), F // TILES
    hbm = pl.BlockSpec(memory_space=pltpu.HBM)
    dma, reg = pltpu.SemaphoreType.DMA, pltpu.SemaphoreType.REGULAR
    v = pltpu.VMEM
    return pl.pallas_call(
        reduce_kernel,
        in_specs=[hbm] * 6,
        out_specs=[hbm] * 4,
        out_shape=[jax.ShapeDtypeStruct(n, BF) for n in ((T, 2 * F), (T, F), (T, W), (F, EXTRA // 2 * FT))],
        scratch_shapes=[
            v((2, M, D), BF), v((2, FT, D), BF), v((2, M, FT), BF), v((2, M, FT), BF),
            v((M, F), BF), v((M, F), BF), v((M, F), BF), v((M, F), BF), v((2, M, FT), BF), v((2, 2 * W, F), BF), v((2, 2 * W, F), BF),
            v((2, M, W), F32), v((4, M, W), BF), v((2, M, W), BF), v((2, 4, M // 2, W), BF), v((2, 3, M // 2, W), BF), v((2, F // 2, FT), BF),
            dma((4,)), dma((4,)), dma((2,)), *[dma((2,))] * 11,
            dma((2,)), dma((4,)), dma((2, 2)), dma((2, 3)), reg((2,)), reg,
        ],
        compiler_params=pltpu.CompilerParams(collective_id=0, has_side_effects=True, vmem_limit_bytes=VMEM_LIMIT),
        name="dx_reduce",
    )(dy, wd, gate, up, wg, wu)


ANY = pl.BlockSpec(memory_space=pl.ANY)
RESIDENT = pl.BlockSpec(memory_space=pltpu.VMEM)


def gate_up_grads(x, dgu, extra, dw_down, bm):
    T, D = x.shape
    F = dgu.shape[1] // 2
    steps = D // bm
    n = extra.shape[1]

    def body(x_ref, d_ref, e_ref, w_ref, og, ou, ow):
        ow[...] = e_ref[...]
        both = tn(x_ref[...], d_ref[...])
        og[...] = both[:, :F].astype(BF)
        ou[...] = both[:, F:].astype(BF)

    some = pl.BlockSpec((F // steps, n), lambda i: (i, 0))
    extra = pltpu.with_memory_space_constraint(extra, pltpu.HBM)
    return pl.pallas_call(
        body,
        grid=(steps,),
        in_specs=[pl.BlockSpec((T, bm), lambda i: (0, i)), RESIDENT, some, ANY],
        out_specs=[pl.BlockSpec((bm, F), lambda i: (i, 0))] * 2 + [some],
        out_shape=[jax.ShapeDtypeStruct((D, F), BF)] * 2 + [jax.ShapeDtypeStruct((F, D), BF)],
        input_output_aliases={3: 2},
        compiler_params=pltpu.CompilerParams(vmem_limit_bytes=26 * 2**20),
        cost_estimate=pl.CostEstimate(flops=4 * T * D * F, bytes_accessed=2 * (T * D + 2 * T * F + 2 * D * F), transcendentals=0),
        name="dw_gate_up",
    )(x, dgu, extra, dw_down)


def down_grad(hid, dy, bn, lo, hi, moved=(), prev=()):
    T, D = dy.shape
    F = hid.shape[1]
    steps = hi - lo

    def body(h_ref, dy_ref, *refs):
        if moved:
            refs[-1][...] = refs[0][...]
        o_ref = refs[-2] if moved else refs[-1]
        o_ref[...] = tn(h_ref[...], dy_ref[...]).astype(BF)

    mb = T // steps
    whole = pl.BlockSpec((T, F), lambda i: (0, 0), pipeline_mode=pl.Buffered(1)) if moved else RESIDENT
    rows = [pl.BlockSpec((mb, D), lambda i: (i, 0))] if moved else []
    return pl.pallas_call(
        body,
        grid=(steps,),
        in_specs=[whole, pl.BlockSpec((T, bn), lambda i: (0, lo + i)), *rows, *[ANY] * len(prev)],
        out_specs=[pl.BlockSpec((F, bn), lambda i: (0, lo + i)), *rows],
        out_shape=[jax.ShapeDtypeStruct((F, D), BF), *[jax.ShapeDtypeStruct((T, D), BF)] * len(moved)],
        input_output_aliases={2 + len(moved): 0} if prev else {},
        compiler_params=pltpu.CompilerParams(vmem_limit_bytes=(36 if moved else 20) * 2**20),
        cost_estimate=pl.CostEstimate(
            flops=2 * T * F * bn * steps,
            bytes_accessed=2 * (T * F + (T + F) * bn * steps + 2 * T * D * len(moved)),
            transcendentals=0,
        ),
        name="dw_down",
    )(hid, dy, *moved, *prev)


def solution(mesh):
    def step(x, dy, gate, up, w_gate, w_up, w_down):
        D = x.shape[1]
        dgu, hid, piece, extra = reduce_call(dy, w_down, gate, up, w_gate, w_up)
        gathered = lax.all_gather(piece, "tp", axis=1, tiled=True)
        bn = D // 16
        (dw_down,) = down_grad(hid, dy, bn, extra.shape[1] // bn, 12)
        dw_gate, dw_up, dw_down = gate_up_grads(x, dgu, extra, dw_down, D // 16)
        dw_down, dx = down_grad(hid, dy, bn // 2, 24, 32, (gathered,), (dw_down,))
        return dx, dw_gate, dw_up, dw_down

    tokens, columns, rows = P("dp", None), P(None, "tp"), P("tp", None)
    return jax.shard_map(
        step,
        mesh=mesh,
        in_specs=(tokens, tokens, P("dp", "tp"), P("dp", "tp"), columns, columns, rows),
        out_specs=(tokens, P("dp", "tp"), P("dp", "tp"), P(("dp", "tp"), None)),
        check_vma=False,
    )
```

```python
import functools

import jax
import jax.numpy as jnp
from jax import lax
from jax.experimental import pallas as pl
from jax.experimental.pallas import tpu as pltpu
from jax.sharding import PartitionSpec as P

BF = jnp.bfloat16
F32 = jnp.float32
VMEM_LIMIT = 67043328
CHUNKS = 4
CHIPS = 8
TILES = 7
STEPS = CHUNKS * CHIPS
SENDS = CHUNKS * (CHIPS - 1)
EXTRA = 8


def nt(a, b):
    return lax.dot_general(a, b, (((1,), (1,)), ((), ())), preferred_element_type=F32)


def tn(a, b):
    return lax.dot_general(a, b, (((0,), (0,)), ((), ())), preferred_element_type=F32)


def chip_at(q):
    return q + (q // 4) * (11 - 2 * q)


def reduce_kernel(
    dy, wd, gate, up, wg, wu,
    dguo, hido, piece, extra,
    dyb, wdb, gtb, utb, dg, du, dgn, dun, hb, wgb, wub, own, precv, psend, rrecv, rsend, fout,
    s_dy, s_fd, s_fo, s_wd, s_gt, s_ut, s_og, s_ou, s_pg, s_pu, s_h, s_dg, s_du, s_fin,
    s_psend, s_precv, s_rsend, s_rrecv, c_ring, c_part,
):
    M, D = dyb.shape[1:]
    W = wgb.shape[1] // 2
    F, FT = dg.shape[1], wdb.shape[1]
    H = M // 2
    i = lax.axis_index("tp")
    core = i % 2
    chip = i // 2
    y = chip // 4
    z = chip % 4
    r = z + y * (7 - 2 * z)
    sgn = 1 - 2 * core
    nxt = {"tp": 2 * chip_at((r + sgn + 8) % 8) + core}
    prv = {"tp": 2 * chip_at((r - sgn + 8) % 8) + core}
    par = {"tp": 2 * chip + 1 - core}
    MESH = pl.DeviceIdType.MESH

    def rows_own(h):
        return pl.multiple_of((2 * chip_at((r - sgn * (1 + h) + 16) % 8) + core) * W, W)

    def rows_par(h):
        return pl.multiple_of((2 * chip_at((r + sgn * (1 + h) + 16) % 8) + 1 - core) * W, W)

    ld = pltpu.make_async_copy

    def own_w(g):
        a, k, half = rows_own(g % 8), g % 2, pl.ds(0, W)
        return [
            ld(wg.at[pl.ds(a, W), :], wgb.at[k, half], s_og.at[k]),
            ld(wu.at[pl.ds(a, W), :], wub.at[k, half], s_ou.at[k]),
        ]

    def par_w(g):
        a, k, half = rows_par(g % 8), (g + 1) % 2, pl.ds(W, W)
        return [
            ld(wg.at[pl.ds(a, W), :], wgb.at[k, half], s_pg.at[k]),
            ld(wu.at[pl.ds(a, W), :], wub.at[k, half], s_pu.at[k]),
        ]

    def dh_place(k):
        c, j = k // TILES, k % TILES
        return pl.ds(pl.multiple_of(c * M, M), M), pl.ds(pl.multiple_of(j * FT, FT), FT)

    def dh_in(k):
        b = k % 2
        rows, cols = dh_place(k)
        return [
            ld(wd.at[cols, :], wdb.at[b], s_wd.at[b]),
            ld(gate.at[rows, cols], gtb.at[b], s_gt.at[b]),
            ld(up.at[rows, cols], utb.at[b], s_ut.at[b]),
        ]

    def dy_in(c, p):
        n = M // 4
        return ld(dy.at[pl.ds(pl.multiple_of(c * M + p * n, n), n), :], dyb.at[c % 2, pl.ds(p * n, n)], s_dy.at[p])

    def dh_out(k, dg, du):
        b = k % 2
        rows, cols = dh_place(k)
        return [
            ld(hb.at[b], hido.at[rows, cols], s_h.at[b]),
            ld(dg.at[:, cols], dguo.at[rows, cols], s_dg.at[b]),
            ld(du.at[:, cols], dguo.at[rows, pl.ds(pl.multiple_of(F + k % TILES * FT, FT), FT)], s_du.at[b]),
        ]

    def extra_in(c):
        n = extra.shape[1]
        return [
            ld(hido.at[pl.ds(c * M, M), :], dyb.at[0, :, pl.ds(c * F, F)], s_dy.at[c]),
            ld(dy.at[pl.ds(c * M, M), pl.ds(0, n)], dyb.at[1, :, pl.ds(c * n, n)], s_fd.at[c]),
        ]

    def extra_out(u):
        rows, cols = pl.ds(pl.multiple_of(u % 2 * (F // 2), F // 2), F // 2), pl.ds(pl.multiple_of(u // 2 * FT, FT), FT)
        return ld(fout.at[u % 2], extra.at[rows, cols], s_fo.at[u % 2])

    def fin(e, c):
        return ld(rsend.at[e, 2], piece.at[pl.ds(pl.multiple_of(c * M + e * H, H), H), :], s_fin.at[e])

    def ring(e, m):
        return pltpu.make_async_remote_copy(
            rsend.at[e, m % 2], rrecv.at[e, m % 3], s_rsend.at[e, m % 2], s_rrecv.at[e, m % 3], device_id=nxt, device_id_type=MESH
        )

    def part(g):
        return pltpu.make_async_remote_copy(
            psend.at[g % 2], precv.at[g % 4], s_psend.at[g % 2], s_precv.at[g % 4], device_id=par, device_id_type=MESH
        )

    def start(copies):
        for c in copies:
            c.start()

    def wait(copies):
        for c in copies:
            c.wait()

    def dh_tile(k, dg, du):
        b, cols = k % 2, dh_place(k)[1]
        d = nt(dyb[(k // TILES) % 2], wdb[b])
        g = gtb[b].astype(F32)
        u = utb[b].astype(F32)
        sig = lax.logistic(g)
        silu = g * sig
        hb[b] = (silu * u).astype(BF)
        du[:, cols] = (d * silu).astype(BF)
        dg[:, cols] = (d * u * (sig * (1.0 + g * (1.0 - sig)))).astype(BF)

    def own_tile(g):
        b, half = g % 2, pl.ds(0, W)
        own[g % 2] = nt(dg[...], wgb[b, half]) + nt(du[...], wub[b, half])

    def par_tile(g, dg, du):
        b, half = (g + 1) % 2, pl.ds(W, W)
        psend[g % 2] = (nt(dg[...], wgb[b, half]) + nt(du[...], wub[b, half])).astype(BF)

    def add(e, g, src, dst):
        rows = pl.ds(e * H, H)
        total = own[g % 2, rows] + precv[(g + 4) % 4, rows].astype(F32) + rrecv[e, src].astype(F32)
        rsend[e, dst] = total.astype(BF)

    def extra_piece(u):
        n, half = extra.shape[1], F // 2
        total = None
        for c in range(CHUNKS):
            h = dyb[0, :, pl.ds(pl.multiple_of(c * F + u % 2 * half, half), half)]
            d = dyb[1, :, pl.ds(pl.multiple_of(c * n + u // 2 * FT, FT), FT)]
            term = tn(h, d)
            total = term if c == 0 else total + term
        fout[u % 2] = total.astype(BF)

    def dh_ready(k):
        wait(dh_in(k))

        @pl.when(k >= 2)
        def _():
            wait(dh_out(k - 2, dg, du))

    def dh_done(k, dg, du):
        start(dh_out(k, dg, du))

        @pl.when(k + 2 < CHUNKS * TILES)
        def _():
            start(dh_in(k + 2))

    start(dh_in(0))
    for p in range(4):
        dy_in(0, p).start()
    start(dh_in(1))
    start(par_w(0))
    start(own_w(0))
    start(par_w(1))
    start(own_w(1))
    barrier = pltpu.get_barrier_semaphore()
    for d in (nxt, prv, par):
        pl.semaphore_signal(barrier, inc=1, device_id=d, device_id_type=MESH)
    for e in range(2):
        rrecv[e, 3] = jnp.zeros((H, W), BF)

    @pl.loop(0, TILES)
    def _(k):
        @pl.when(k == 0)
        def _():
            for p in range(4):
                dy_in(0, p).wait()

        dh_ready(k)
        dh_tile(k, dg, du)
        dh_done(k, dg, du)

        @pl.when(k < 4)
        def _():
            dy_in(1, k).start()

    wait(par_w(0))
    par_tile(0, dg, du)
    pl.semaphore_wait(barrier, 3)
    part(0).start()
    start(par_w(2))

    @pl.loop(0, STEPS)
    def _(t):
        c, s = t // 8, t % 8
        has_dh = (s < 7) & (c < CHUNKS - 1)
        k = TILES * (c + 1) + s
        g = t - 1
        h = (g + 8) % 8
        m = 7 * ((g + 8) // 8 - 1) + h
        adds = t >= 1
        takes = adds & (h >= 1)
        sends = adds & (h <= 6)
        ends = adds & (h == 7)
        last = (h + 1) // 8
        got = (h + 7) // 8 * (1 - (STEPS - t) // STEPS)
        src = got * ((m + 2) % 3) + (1 - got) * 3
        dst = (1 - last) * (m % 2) + last * 2

        wait(own_w(t))

        @pl.when(t + 1 < STEPS)
        def _():
            wait(par_w(t + 1))

        @pl.when((s == 0) & (c < CHUNKS - 1))
        def _():
            for p in range(4):
                dy_in(c + 1, p).wait()

        @pl.when(has_dh)
        def _():
            dh_ready(k)

        @pl.when(adds)
        def _():
            part(g).wait_recv()
            part(g).wait_send()

        @pl.when(sends & (m >= 2))
        def _():
            for e in range(2):
                ring(e, m - 2).wait_send()

        @pl.when(sends & (m >= 3))
        def _():
            for e in range(2):
                pl.semaphore_wait(c_ring.at[e], 1)

        @pl.when(ends & (t >= 16))
        def _():
            for e in range(2):
                fin(e, c - 2).wait()

        def pass_on(e):
            @pl.when(takes)
            def _():
                ring(e, m - 1).wait_recv()

            add(e, g, src, dst)

            @pl.when(sends)
            def _():
                ring(e, m).start()

        pass_on(0)

        @pl.when(has_dh)
        def _():
            dh_tile(k, dgn, dun)

        @pl.when(jnp.logical_not(has_dh))
        def _():
            own_tile(t)

        pass_on(1)

        @pl.when(has_dh)
        def _():
            own_tile(t)
            par_tile(t + 1, dg, du)
            dh_done(k, dgn, dun)

        @pl.when((s < 7) & (c == CHUNKS - 1))
        def _():
            @pl.when(s == 0)
            def _():
                for b in range(CHUNKS):
                    wait(extra_in(b))

            @pl.when(s >= 2)
            def _():
                extra_out(s - 2).wait()

            par_tile(t + 1, dg, du)
            extra_piece(s)
            extra_out(s).start()

        @pl.when((s == 7) & (c < CHUNKS - 1))
        def _():
            par_tile(t + 1, dgn, dun)
            dg[...] = dgn[...]
            du[...] = dun[...]

        @pl.when(ends)
        def _():
            for e in range(2):
                fin(e, c - 1).start()

        @pl.when(t + 1 < STEPS)
        def _():
            @pl.when(t >= 2)
            def _():
                pl.semaphore_wait(c_part, 1)

            part(t + 1).start()

        @pl.when(takes & (m - 1 < SENDS - 3))
        def _():
            for e in range(2):
                pl.semaphore_signal(c_ring.at[e], inc=1, device_id=prv, device_id_type=MESH)

        @pl.when(t < STEPS - 3)
        def _():
            pl.semaphore_signal(c_part, inc=1, device_id=par, device_id_type=MESH)

        @pl.when((s < 4) & (c < CHUNKS - 2))
        def _():
            dy_in(c + 2, s).start()

        @pl.when(t + 2 < STEPS)
        def _():
            start(own_w(t + 2))

        @pl.when(t + 3 < STEPS)
        def _():
            start(par_w(t + 3))

        @pl.when(t == 8 * (CHUNKS - 2) + 2)
        def _():
            for b in range(CHUNKS - 1):
                extra_in(b)[0].start()

        @pl.when(t == 8 * (CHUNKS - 1) - 2)
        def _():
            for b in range(CHUNKS):
                extra_in(b)[1].start()

        @pl.when(t == 8 * (CHUNKS - 1) - 1)
        def _():
            for k in (CHUNKS * TILES - 2, CHUNKS * TILES - 1):
                wait(dh_out(k, dgn, dun))
            extra_in(CHUNKS - 1)[0].start()

    part(STEPS - 1).wait_recv()
    part(STEPS - 1).wait_send()
    for e in range(2):
        fin(e, CHUNKS - 2).wait()
        if e == 1:
            extra_out(EXTRA - 3).wait()
            extra_piece(EXTRA - 1)
            extra_out(EXTRA - 1).start()
        ring(e, SENDS - 1).wait_recv()
        add(e, STEPS - 1, (SENDS - 1) % 3, 2)
        fin(e, CHUNKS - 1).start()
    for e in range(2):
        ring(e, SENDS - 2).wait_send()
        ring(e, SENDS - 1).wait_send()
        fin(e, CHUNKS - 1).wait()
    extra_out(EXTRA - 2).wait()
    extra_out(EXTRA - 1).wait()


def reduce_call(dy, wd, gate, up, wg, wu):
    T, D = dy.shape
    F = gate.shape[1]
    M, W, FT = T // CHUNKS, D // (2 * CHIPS), F // TILES
    hbm = pl.BlockSpec(memory_space=pltpu.HBM)
    dma, reg = pltpu.SemaphoreType.DMA, pltpu.SemaphoreType.REGULAR
    v = pltpu.VMEM
    return pl.pallas_call(
        reduce_kernel,
        in_specs=[hbm] * 6,
        out_specs=[hbm] * 4,
        out_shape=[jax.ShapeDtypeStruct(n, BF) for n in ((T, 2 * F), (T, F), (T, W), (F, EXTRA // 2 * FT))],
        scratch_shapes=[
            v((2, M, D), BF), v((2, FT, D), BF), v((2, M, FT), BF), v((2, M, FT), BF),
            v((M, F), BF), v((M, F), BF), v((M, F), BF), v((M, F), BF), v((2, M, FT), BF), v((2, 2 * W, F), BF), v((2, 2 * W, F), BF),
            v((2, M, W), F32), v((4, M, W), BF), v((2, M, W), BF), v((2, 4, M // 2, W), BF), v((2, 3, M // 2, W), BF), v((2, F // 2, FT), BF),
            dma((4,)), dma((4,)), dma((2,)), *[dma((2,))] * 11,
            dma((2,)), dma((4,)), dma((2, 2)), dma((2, 3)), reg((2,)), reg,
        ],
        compiler_params=pltpu.CompilerParams(collective_id=0, has_side_effects=True, vmem_limit_bytes=VMEM_LIMIT),
        name="dx_reduce",
    )(dy, wd, gate, up, wg, wu)


ANY = pl.BlockSpec(memory_space=pl.ANY)
RESIDENT = pl.BlockSpec(memory_space=pltpu.VMEM)


def gate_up_grads(x, dgu, extra, dw_down, bm):
    T, D = x.shape
    F = dgu.shape[1] // 2
    steps = D // bm
    n = extra.shape[1]

    def body(x_ref, d_ref, e_ref, w_ref, og, ou, ow):
        ow[...] = e_ref[...]
        both = tn(x_ref[...], d_ref[...])
        og[...] = both[:, :F].astype(BF)
        ou[...] = both[:, F:].astype(BF)

    some = pl.BlockSpec((F // steps, n), lambda i: (i, 0))
    extra = pltpu.with_memory_space_constraint(extra, pltpu.HBM)
    return pl.pallas_call(
        body,
        grid=(steps,),
        in_specs=[pl.BlockSpec((T, bm), lambda i: (0, i)), RESIDENT, some, ANY],
        out_specs=[pl.BlockSpec((bm, F), lambda i: (i, 0))] * 2 + [some],
        out_shape=[jax.ShapeDtypeStruct((D, F), BF)] * 2 + [jax.ShapeDtypeStruct((F, D), BF)],
        input_output_aliases={3: 2},
        compiler_params=pltpu.CompilerParams(vmem_limit_bytes=26 * 2**20),
        cost_estimate=pl.CostEstimate(flops=4 * T * D * F, bytes_accessed=2 * (T * D + 2 * T * F + 2 * D * F), transcendentals=0),
        name="dw_gate_up",
    )(x, dgu, extra, dw_down)


def down_kernel(lo, steps, moving, *refs):
    if moving:
        hid, dy, src, _, out, dst, hidb, dyb, ob, cb, s_h, s_d, s_o, s_in, s_out = refs
    else:
        hid, dy, out, hidb, dyb, ob, acc, s_h, s_d, s_o = refs
    ld = pltpu.make_async_copy
    T = hid.shape[0]
    bn = dyb.shape[2]
    half = T // 2

    def cols(i):
        return pl.ds(pl.multiple_of((lo + i) * bn, bn), bn)

    def h_in(p):
        rows = pl.ds(p * half, half)
        return ld(hid.at[rows, :], hidb.at[rows, :], s_h.at[p])

    def dy_in(i, p):
        rows = pl.ds(p * half, half)
        return ld(dy.at[rows, cols(i)], dyb.at[i % 2, rows], s_d.at[i % 2, p])

    def put(i):
        return ld(ob.at[i % 2], out.at[:, cols(i)], s_o.at[i % 2])

    if moving:
        n = cb.shape[1]

        def rows_at(k):
            return pl.ds(pl.multiple_of(k * n, n), n)

        def come(k):
            return ld(src.at[rows_at(k), :], cb.at[k % 8], s_in.at[k % 8])

        def go(k):
            return ld(cb.at[k % 8], dst.at[rows_at(k), :], s_out.at[k % 8])

    for p in range(2):
        h_in(p).start()
        dy_in(0, p).start()
    if moving:
        for k in range(4):
            come(k).start()
    for p in range(2):
        dy_in(1, p).start()

    def block(i):
        for p in range(2):
            dy_in(i, p).wait()

        @pl.when(i >= 2)
        def _():
            put(i - 2).wait()

        if moving:
            for e in range(2):
                come(2 * i + e).wait()
                go(2 * i + e).start()

            @pl.when(i >= 2)
            def _():
                for e in range(2):
                    go(2 * i - 4 + e).wait()

            @pl.when(i + 2 < steps)
            def _():
                for e in range(2):
                    come(2 * i + 4 + e).start()

        ob[i % 2] = tn(hidb[...], dyb[i % 2]).astype(BF)
        end(i)

    def end(i):
        put(i).start()

        @pl.when(i + 2 < steps)
        def _():
            for p in range(2):
                dy_in(i + 2, p).start()

    if moving:
        for p in range(2):
            h_in(p).wait()
        pl.loop(0, steps)(block)
        for k in range(2 * steps - 4, 2 * steps):
            go(k).wait()
    else:
        for p in range(2):
            h_in(p).wait()
            dy_in(0, p).wait()
            rows = pl.ds(p * half, half)
            term = tn(hidb[rows], dyb[0, rows])
            if p == 0:
                acc[...] = term
            else:
                ob[0] = (acc[...] + term).astype(BF)
        end(0)
        pl.loop(1, steps)(block)
    put(steps - 2).wait()
    put(steps - 1).wait()


def down_grad(hid, dy, bn, lo, hi, moved=(), prev=()):
    T, D = dy.shape
    F = hid.shape[1]
    steps = hi - lo
    hbm = pl.BlockSpec(memory_space=pltpu.HBM)
    dma, v = pltpu.SemaphoreType.DMA, pltpu.VMEM
    hid, dy = (pltpu.with_memory_space_constraint(a, pltpu.HBM) for a in (hid, dy))
    scratch = [v((T, F), BF), v((2, T, bn), BF), v((2, F, bn), BF)]
    scratch.append(v((8, T // (2 * steps), D), BF) if moved else v((F, bn), F32))
    scratch += [dma((2,)), dma((2, 2)), dma((2,))] + [dma((8,))] * (2 * len(moved))
    return pl.pallas_call(
        functools.partial(down_kernel, lo, steps, bool(moved)),
        in_specs=[hbm] * (2 + len(moved) + len(prev)),
        out_specs=[hbm] * (1 + len(moved)),
        out_shape=[jax.ShapeDtypeStruct((F, D), BF), *[jax.ShapeDtypeStruct((T, D), BF)] * len(moved)],
        scratch_shapes=scratch,
        input_output_aliases={2 + len(moved): 0} if prev else {},
        compiler_params=pltpu.CompilerParams(vmem_limit_bytes=(48 if moved else 30) * 2**20),
        cost_estimate=pl.CostEstimate(
            flops=2 * T * F * bn * steps,
            bytes_accessed=2 * (T * F + (T + F) * bn * steps + 2 * T * D * len(moved)),
            transcendentals=0,
        ),
        name="dw_down",
    )(hid, dy, *moved, *prev)


def solution(mesh):
    def step(x, dy, gate, up, w_gate, w_up, w_down):
        D = x.shape[1]
        dgu, hid, piece, extra = reduce_call(dy, w_down, gate, up, w_gate, w_up)
        gathered = lax.all_gather(piece, "tp", axis=1, tiled=True)
        bn = D // 16
        (dw_down,) = down_grad(hid, dy, bn, extra.shape[1] // bn, 12)
        dw_gate, dw_up, dw_down = gate_up_grads(x, dgu, extra, dw_down, D // 16)
        dw_down, dx = down_grad(hid, dy, bn // 2, 24, 32, (gathered,), (dw_down,))
        return dx, dw_gate, dw_up, dw_down

    tokens, columns, rows = P("dp", None), P(None, "tp"), P("tp", None)
    return jax.shard_map(
        step,
        mesh=mesh,
        in_specs=(tokens, tokens, P("dp", "tp"), P("dp", "tp"), columns, columns, rows),
        out_specs=(tokens, P("dp", "tp"), P("dp", "tp"), P(("dp", "tp"), None)),
        check_vma=False,
    )
```

```python
import functools

import jax
import jax.numpy as jnp
from jax import lax
from jax.experimental import pallas as pl
from jax.experimental.pallas import tpu as pltpu
from jax.sharding import PartitionSpec as P

BF = jnp.bfloat16
F32 = jnp.float32
VMEM_LIMIT = 67043328
CHUNKS = 4
CHIPS = 8
TILES = 7
STEPS = CHUNKS * CHIPS
SENDS = CHUNKS * (CHIPS - 1)
EXTRA = 12


def nt(a, b):
    return lax.dot_general(a, b, (((1,), (1,)), ((), ())), preferred_element_type=F32)


def tn(a, b):
    return lax.dot_general(a, b, (((0,), (0,)), ((), ())), preferred_element_type=F32)


def chip_at(q):
    return q + (q // 4) * (11 - 2 * q)


def reduce_kernel(
    dy, wd, gate, up, wg, wu,
    dguo, hido, piece, extra,
    dyb, wdb, gtb, utb, dg, du, dgn, dun, hb, wgb, wub, own, precv, psend, rrecv, rsend, fout,
    s_dy, s_fd, s_fo, s_wd, s_gt, s_ut, s_og, s_ou, s_pg, s_pu, s_h, s_dg, s_du, s_fin,
    s_psend, s_precv, s_rsend, s_rrecv, c_ring, c_part,
):
    M, D = dyb.shape[1:]
    W = wgb.shape[1] // 2
    F, FT = dg.shape[1], wdb.shape[1]
    H = M // 2
    i = lax.axis_index("tp")
    core = i % 2
    chip = i // 2
    y = chip // 4
    z = chip % 4
    r = z + y * (7 - 2 * z)
    sgn = 1 - 2 * core
    nxt = {"tp": 2 * chip_at((r + sgn + 8) % 8) + core}
    prv = {"tp": 2 * chip_at((r - sgn + 8) % 8) + core}
    par = {"tp": 2 * chip + 1 - core}
    MESH = pl.DeviceIdType.MESH

    def rows_own(h):
        return pl.multiple_of((2 * chip_at((r - sgn * (1 + h) + 16) % 8) + core) * W, W)

    def rows_par(h):
        return pl.multiple_of((2 * chip_at((r + sgn * (1 + h) + 16) % 8) + 1 - core) * W, W)

    ld = pltpu.make_async_copy

    def own_w(g):
        a, k, half = rows_own(g % 8), g % 2, pl.ds(0, W)
        return [
            ld(wg.at[pl.ds(a, W), :], wgb.at[k, half], s_og.at[k]),
            ld(wu.at[pl.ds(a, W), :], wub.at[k, half], s_ou.at[k]),
        ]

    def par_w(g):
        a, k, half = rows_par(g % 8), (g + 1) % 2, pl.ds(W, W)
        return [
            ld(wg.at[pl.ds(a, W), :], wgb.at[k, half], s_pg.at[k]),
            ld(wu.at[pl.ds(a, W), :], wub.at[k, half], s_pu.at[k]),
        ]

    def dh_place(k):
        c, j = k // TILES, k % TILES
        return pl.ds(pl.multiple_of(c * M, M), M), pl.ds(pl.multiple_of(j * FT, FT), FT)

    def dh_in(k):
        b = k % 2
        rows, cols = dh_place(k)
        return [
            ld(wd.at[cols, :], wdb.at[b], s_wd.at[b]),
            ld(gate.at[rows, cols], gtb.at[b], s_gt.at[b]),
            ld(up.at[rows, cols], utb.at[b], s_ut.at[b]),
        ]

    def dy_in(c, p):
        n = M // 4
        return ld(dy.at[pl.ds(pl.multiple_of(c * M + p * n, n), n), :], dyb.at[c % 2, pl.ds(p * n, n)], s_dy.at[p])

    def dh_out(k, dg, du):
        b = k % 2
        rows, cols = dh_place(k)
        return [
            ld(hb.at[b], hido.at[rows, cols], s_h.at[b]),
            ld(dg.at[:, cols], dguo.at[rows, cols], s_dg.at[b]),
            ld(du.at[:, cols], dguo.at[rows, pl.ds(pl.multiple_of(F + k % TILES * FT, FT), FT)], s_du.at[b]),
        ]

    def extra_in(c):
        n = extra.shape[1]
        return [
            ld(hido.at[pl.ds(c * M, M), :], dyb.at[0, :, pl.ds(c * F, F)], s_dy.at[c]),
            ld(dy.at[pl.ds(c * M, M), pl.ds(0, n)], dyb.at[1, :, pl.ds(c * n, n)], s_fd.at[c]),
        ]

    def extra_out(u):
        rows, cols = pl.ds(pl.multiple_of(u % 2 * (F // 2), F // 2), F // 2), pl.ds(pl.multiple_of(u // 2 * FT, FT), FT)
        return ld(fout.at[u % 2], extra.at[rows, cols], s_fo.at[u % 2])

    def fin(e, c):
        return ld(rsend.at[e, 2], piece.at[pl.ds(pl.multiple_of(c * M + e * H, H), H), :], s_fin.at[e])

    def ring(e, m):
        return pltpu.make_async_remote_copy(
            rsend.at[e, m % 2], rrecv.at[e, m % 3], s_rsend.at[e, m % 2], s_rrecv.at[e, m % 3], device_id=nxt, device_id_type=MESH
        )

    def part(g):
        return pltpu.make_async_remote_copy(
            psend.at[g % 2], precv.at[g % 4], s_psend.at[g % 2], s_precv.at[g % 4], device_id=par, device_id_type=MESH
        )

    def start(copies):
        for c in copies:
            c.start()

    def wait(copies):
        for c in copies:
            c.wait()

    def dh_tile(k, dg, du):
        b, cols = k % 2, dh_place(k)[1]
        d = nt(dyb[(k // TILES) % 2], wdb[b])
        g = gtb[b].astype(F32)
        u = utb[b].astype(F32)
        sig = lax.logistic(g)
        silu = g * sig
        hb[b] = (silu * u).astype(BF)
        du[:, cols] = (d * silu).astype(BF)
        dg[:, cols] = (d * u * (sig * (1.0 + g * (1.0 - sig)))).astype(BF)

    def own_tile(g):
        b, half = g % 2, pl.ds(0, W)
        term = nt(dg[...], wgb[b, half]) + nt(du[...], wub[b, half])
        own[g % 2] = term + precv[g % 4].astype(F32)

    def par_tile(g, dg, du):
        b, half = (g + 1) % 2, pl.ds(W, W)
        psend[g % 2] = (nt(dg[...], wgb[b, half]) + nt(du[...], wub[b, half])).astype(BF)

    def add(e, g, src, dst):
        total = own[g % 2, pl.ds(e * H, H)] + rrecv[e, src].astype(F32)
        rsend[e, dst] = total.astype(BF)

    def extra_piece(u):
        n, half = extra.shape[1], F // 2
        total = None
        for c in range(CHUNKS):
            h = dyb[0, :, pl.ds(pl.multiple_of(c * F + u % 2 * half, half), half)]
            d = dyb[1, :, pl.ds(pl.multiple_of(c * n + u // 2 * FT, FT), FT)]
            term = tn(h, d)
            total = term if c == 0 else total + term
        fout[u % 2] = total.astype(BF)

    def dh_ready(k, early=False):
        wait(dh_in(k))
        if early:
            pl.when(k >= 2)(lambda: wait(dh_out(k - 2, dg, du)))
        else:
            wait(dh_out(k - 2, dg, du))

    def dh_done(k, dg, du):
        start(dh_out(k, dg, du))

        @pl.when(k + 2 < CHUNKS * TILES)
        def _():
            start(dh_in(k + 2))

    start(dh_in(0))
    for p in range(4):
        dy_in(0, p).start()
    start(dh_in(1))
    start(par_w(0))
    start(own_w(0))
    start(par_w(1))
    start(own_w(1))
    barrier = pltpu.get_barrier_semaphore()
    for d in (nxt, prv, par):
        pl.semaphore_signal(barrier, inc=1, device_id=d, device_id_type=MESH)
    for e in range(2):
        rrecv[e, 3] = jnp.zeros((H, W), BF)

    @pl.loop(0, TILES)
    def _(k):
        @pl.when(k == 0)
        def _():
            for p in range(4):
                dy_in(0, p).wait()

        dh_ready(k, early=True)
        dh_tile(k, dg, du)
        dh_done(k, dg, du)

        @pl.when(k < 4)
        def _():
            dy_in(1, k).start()

    wait(par_w(0))
    par_tile(0, dg, du)
    pl.semaphore_wait(barrier, 3)
    part(0).start()
    start(par_w(2))

    @pl.loop(0, STEPS)
    def _(t):
        c, s = t // 8, t % 8
        has_dh = (s < 7) & (c < CHUNKS - 1)
        k = TILES * (c + 1) + s
        g = t - 1
        h = (g + 8) % 8
        m = 7 * ((g + 8) // 8 - 1) + h
        adds = t >= 1
        takes = adds & (h >= 1)
        sends = adds & (h <= 6)
        ends = adds & (h == 7)
        last = (h + 1) // 8
        got = (h + 7) // 8 * (1 - (STEPS - t) // STEPS)
        src = got * ((m + 2) % 3) + (1 - got) * 3
        dst = (1 - last) * (m % 2) + last * 2

        @pl.when(has_dh)
        def _():
            dh_ready(k)

        @pl.when(jnp.logical_not(has_dh))
        def _():
            wait(own_w(t))

            @pl.when(t + 1 < STEPS)
            def _():
                wait(par_w(t + 1))

        @pl.when(s == 0)
        def _():
            @pl.when(c < CHUNKS - 1)
            def _():
                for p in range(4):
                    dy_in(c + 1, p).wait()

            @pl.when(t >= 16)
            def _():
                for e in range(2):
                    fin(e, c - 2).wait()

        @pl.when(adds)
        def _():
            part(g).wait_send()

        @pl.when(sends)
        def _():
            @pl.when(m >= 2)
            def _():
                for e in range(2):
                    ring(e, m - 2).wait_send()

            @pl.when(m >= 3)
            def _():
                for e in range(2):
                    pl.semaphore_wait(c_ring.at[e], 1)

        def pass_on(e):
            @pl.when(takes)
            def _():
                ring(e, m - 1).wait_recv()

            add(e, g, src, dst)

            @pl.when(sends)
            def _():
                ring(e, m).start()

        pass_on(0)

        @pl.when(has_dh)
        def _():
            dh_tile(k, dgn, dun)

        @pl.when((s < 7) & (c == CHUNKS - 1))
        def _():
            @pl.when(s == 0)
            def _():
                for b in range(CHUNKS):
                    wait(extra_in(b))

            @pl.when(s >= 2)
            def _():
                extra_out(s - 2).wait()

            par_tile(t + 1, dg, du)
            extra_piece(s)
            extra_out(s).start()

        @pl.when((s == 7) & (c < CHUNKS - 1))
        def _():
            par_tile(t + 1, dgn, dun)

        pass_on(1)

        @pl.when(has_dh)
        def _():
            wait(own_w(t))
            wait(par_w(t + 1))
            part(t).wait_recv()
            own_tile(t)
            par_tile(t + 1, dg, du)
            dh_done(k, dgn, dun)
            start(own_w(t + 2))
            start(par_w(t + 3))

        @pl.when(jnp.logical_not(has_dh))
        def _():
            part(t).wait_recv()
            own_tile(t)

            @pl.when((s == 7) & (c < CHUNKS - 1))
            def _():
                dg[...] = dgn[...]
                du[...] = dun[...]

            @pl.when(t + 2 < STEPS)
            def _():
                start(own_w(t + 2))

            @pl.when(t + 3 < STEPS)
            def _():
                start(par_w(t + 3))

        @pl.when(ends)
        def _():
            for e in range(2):
                fin(e, c - 1).start()

        @pl.when(t + 1 < STEPS)
        def _():
            @pl.when(t >= 2)
            def _():
                pl.semaphore_wait(c_part, 1)

            part(t + 1).start()

        @pl.when(takes & (m - 1 < SENDS - 3))
        def _():
            for e in range(2):
                pl.semaphore_signal(c_ring.at[e], inc=1, device_id=prv, device_id_type=MESH)

        @pl.when(t < STEPS - 3)
        def _():
            pl.semaphore_signal(c_part, inc=1, device_id=par, device_id_type=MESH)

        @pl.when((s < 4) & (c < CHUNKS - 2))
        def _():
            dy_in(c + 2, s).start()

        @pl.when(c == CHUNKS - 2)
        def _():
            @pl.when(s == 2)
            def _():
                for b in range(CHUNKS - 1):
                    extra_in(b)[0].start()

            @pl.when(s == 6)
            def _():
                for b in range(CHUNKS):
                    extra_in(b)[1].start()

            @pl.when(s == 7)
            def _():
                for k in (CHUNKS * TILES - 2, CHUNKS * TILES - 1):
                    wait(dh_out(k, dgn, dun))
                extra_in(CHUNKS - 1)[0].start()

    part(STEPS - 1).wait_send()

    @pl.loop(7, EXTRA)
    def _(u):
        extra_out(u - 2).wait()
        extra_piece(u)
        extra_out(u).start()

        @pl.when(u >= EXTRA - 2)
        def _():
            e = u - (EXTRA - 2)
            fin(e, CHUNKS - 2).wait()
            ring(e, SENDS - 1).wait_recv()
            add(e, STEPS - 1, (SENDS - 1) % 3, 2)
            fin(e, CHUNKS - 1).start()

    for e in range(2):
        ring(e, SENDS - 2).wait_send()
        ring(e, SENDS - 1).wait_send()
        fin(e, CHUNKS - 1).wait()
    extra_out(EXTRA - 2).wait()
    extra_out(EXTRA - 1).wait()


def reduce_call(dy, wd, gate, up, wg, wu):
    T, D = dy.shape
    F = gate.shape[1]
    M, W, FT = T // CHUNKS, D // (2 * CHIPS), F // TILES
    hbm = pl.BlockSpec(memory_space=pltpu.HBM)
    dma, reg = pltpu.SemaphoreType.DMA, pltpu.SemaphoreType.REGULAR
    v = pltpu.VMEM
    return pl.pallas_call(
        reduce_kernel,
        in_specs=[hbm] * 6,
        out_specs=[hbm] * 4,
        out_shape=[jax.ShapeDtypeStruct(n, BF) for n in ((T, 2 * F), (T, F), (T, W), (F, EXTRA // 2 * FT))],
        scratch_shapes=[
            v((2, M, D), BF), v((2, FT, D), BF), v((2, M, FT), BF), v((2, M, FT), BF),
            v((M, F), BF), v((M, F), BF), v((M, F), BF), v((M, F), BF), v((2, M, FT), BF), v((2, 2 * W, F), BF), v((2, 2 * W, F), BF),
            v((2, M, W), F32), v((4, M, W), BF), v((2, M, W), BF), v((2, 4, M // 2, W), BF), v((2, 3, M // 2, W), BF), v((2, F // 2, FT), BF),
            dma((4,)), dma((4,)), dma((2,)), *[dma((2,))] * 11,
            dma((2,)), dma((4,)), dma((2, 2)), dma((2, 3)), reg((2,)), reg,
        ],
        compiler_params=pltpu.CompilerParams(collective_id=0, has_side_effects=True, vmem_limit_bytes=VMEM_LIMIT),
        name="dx_reduce",
    )(dy, wd, gate, up, wg, wu)


ANY = pl.BlockSpec(memory_space=pl.ANY)
RESIDENT = pl.BlockSpec(memory_space=pltpu.VMEM)


def gate_up_grads(x, dgu, extra, dw_down, bm):
    T, D = x.shape
    F = dgu.shape[1] // 2
    steps = D // bm
    n = extra.shape[1]

    def body(x_ref, d_ref, e_ref, w_ref, og, ou, ow):
        ow[...] = e_ref[...]
        both = tn(x_ref[...], d_ref[...])
        og[...] = both[:, :F].astype(BF)
        ou[...] = both[:, F:].astype(BF)

    some = pl.BlockSpec((F // steps, n), lambda i: (i, 0))
    extra = pltpu.with_memory_space_constraint(extra, pltpu.HBM)
    return pl.pallas_call(
        body,
        grid=(steps,),
        in_specs=[pl.BlockSpec((T, bm), lambda i: (0, i)), RESIDENT, some, ANY],
        out_specs=[pl.BlockSpec((bm, F), lambda i: (i, 0))] * 2 + [some],
        out_shape=[jax.ShapeDtypeStruct((D, F), BF)] * 2 + [jax.ShapeDtypeStruct((F, D), BF)],
        input_output_aliases={3: 2},
        compiler_params=pltpu.CompilerParams(vmem_limit_bytes=26 * 2**20),
        cost_estimate=pl.CostEstimate(flops=4 * T * D * F, bytes_accessed=2 * (T * D + 2 * T * F + 2 * D * F), transcendentals=0),
        name="dw_gate_up",
    )(x, dgu, extra, dw_down)


def down_kernel(lo, steps, moving, *refs):
    if moving:
        hid, dy, src, _, out, dst, hidb, dyb, ob, cb, s_h, s_d, s_o, s_in, s_out = refs
    else:
        hid, dy, out, hidb, dyb, ob, acc, s_h, s_d, s_o = refs
    ld = pltpu.make_async_copy
    T = hid.shape[0]
    bn = dyb.shape[2]
    half = T // 2

    def cols(i):
        return pl.ds(pl.multiple_of((lo + i) * bn, bn), bn)

    def h_in(p):
        rows = pl.ds(p * half, half)
        return ld(hid.at[rows, :], hidb.at[rows, :], s_h.at[p])

    def dy_in(i, p):
        rows = pl.ds(p * half, half)
        return ld(dy.at[rows, cols(i)], dyb.at[i % 2, rows], s_d.at[i % 2, p])

    def put(i):
        return ld(ob.at[i % 2], out.at[:, cols(i)], s_o.at[i % 2])

    if moving:
        n = cb.shape[1]

        def rows_at(k):
            return pl.ds(pl.multiple_of(k * n, n), n)

        def come(k):
            return ld(src.at[rows_at(k), :], cb.at[k % 8], s_in.at[k % 8])

        def go(k):
            return ld(cb.at[k % 8], dst.at[rows_at(k), :], s_out.at[k % 8])

    for p in range(2):
        h_in(p).start()
        dy_in(0, p).start()
    if moving:
        for k in range(4):
            come(k).start()
    for p in range(2):
        dy_in(1, p).start()

    def block(i):
        for p in range(2):
            dy_in(i, p).wait()

        @pl.when(i >= 2)
        def _():
            put(i - 2).wait()

        if moving:
            for e in range(2):
                come(2 * i + e).wait()
                go(2 * i + e).start()

            @pl.when(i >= 2)
            def _():
                for e in range(2):
                    go(2 * i - 4 + e).wait()

            @pl.when(i + 2 < steps)
            def _():
                for e in range(2):
                    come(2 * i + 4 + e).start()

        ob[i % 2] = tn(hidb[...], dyb[i % 2]).astype(BF)
        end(i)

    def end(i):
        put(i).start()

        @pl.when(i + 2 < steps)
        def _():
            for p in range(2):
                dy_in(i + 2, p).start()

    if moving:
        for p in range(2):
            h_in(p).wait()
        pl.loop(0, steps)(block)
        for k in range(2 * steps - 4, 2 * steps):
            go(k).wait()
    else:
        for p in range(2):
            h_in(p).wait()
            dy_in(0, p).wait()
            rows = pl.ds(p * half, half)
            term = tn(hidb[rows], dyb[0, rows])
            if p == 0:
                acc[...] = term
            else:
                ob[0] = (acc[...] + term).astype(BF)
        end(0)
        pl.loop(1, steps)(block)
    put(steps - 2).wait()
    put(steps - 1).wait()


def down_grad(hid, dy, bn, lo, hi, moved=(), prev=()):
    T, D = dy.shape
    F = hid.shape[1]
    steps = hi - lo
    hbm = pl.BlockSpec(memory_space=pltpu.HBM)
    dma, v = pltpu.SemaphoreType.DMA, pltpu.VMEM
    hid, dy = (pltpu.with_memory_space_constraint(a, pltpu.HBM) for a in (hid, dy))
    scratch = [v((T, F), BF), v((2, T, bn), BF), v((2, F, bn), BF)]
    scratch.append(v((8, T // (2 * steps), D), BF) if moved else v((F, bn), F32))
    scratch += [dma((2,)), dma((2, 2)), dma((2,))] + [dma((8,))] * (2 * len(moved))
    return pl.pallas_call(
        functools.partial(down_kernel, lo, steps, bool(moved)),
        in_specs=[hbm] * (2 + len(moved) + len(prev)),
        out_specs=[hbm] * (1 + len(moved)),
        out_shape=[jax.ShapeDtypeStruct((F, D), BF), *[jax.ShapeDtypeStruct((T, D), BF)] * len(moved)],
        scratch_shapes=scratch,
        input_output_aliases={2 + len(moved): 0} if prev else {},
        compiler_params=pltpu.CompilerParams(vmem_limit_bytes=(48 if moved else 30) * 2**20),
        cost_estimate=pl.CostEstimate(
            flops=2 * T * F * bn * steps,
            bytes_accessed=2 * (T * F + (T + F) * bn * steps + 2 * T * D * len(moved)),
            transcendentals=0,
        ),
        name="dw_down",
    )(hid, dy, *moved, *prev)


def solution(mesh):
    def step(x, dy, gate, up, w_gate, w_up, w_down):
        D = x.shape[1]
        dgu, hid, piece, extra = reduce_call(dy, w_down, gate, up, w_gate, w_up)
        gathered = lax.all_gather(piece, "tp", axis=1, tiled=True)
        bn = D // 16
        (dw_down,) = down_grad(hid, dy, bn, extra.shape[1] // bn, 12)
        dw_gate, dw_up, dw_down = gate_up_grads(x, dgu, extra, dw_down, D // 16)
        dw_down, dx = down_grad(hid, dy, bn // 2, 24, 32, (gathered,), (dw_down,))
        return dx, dw_gate, dw_up, dw_down

    tokens, columns, rows = P("dp", None), P(None, "tp"), P("tp", None)
    return jax.shard_map(
        step,
        mesh=mesh,
        in_specs=(tokens, tokens, P("dp", "tp"), P("dp", "tp"), columns, columns, rows),
        out_specs=(tokens, P("dp", "tp"), P("dp", "tp"), P(("dp", "tp"), None)),
        check_vma=False,
    )
```

```python
import functools

import jax
import jax.numpy as jnp
from jax import lax
from jax.experimental import pallas as pl
from jax.experimental.pallas import tpu as pltpu
from jax.sharding import PartitionSpec as P

BF = jnp.bfloat16
F32 = jnp.float32
VMEM_LIMIT = 67043328
CHUNKS = 4
CHIPS = 8
TILES = 7
STEPS = CHUNKS * CHIPS
SENDS = CHUNKS * (CHIPS - 1)
EXTRA = 12


def nt(a, b):
    return lax.dot_general(a, b, (((1,), (1,)), ((), ())), preferred_element_type=F32)


def tn(a, b):
    return lax.dot_general(a, b, (((0,), (0,)), ((), ())), preferred_element_type=F32)


def chip_at(q):
    return q + (q // 4) * (11 - 2 * q)


def reduce_kernel(
    dy, wd, gate, up, wg, wu,
    dguo, hido, piece, extra,
    dyb, wdb, gtb, utb, dg, du, dgn, dun, hb, wgb, wub, own, precv, psend, rrecv, rsend, fout,
    s_dy, s_fd, s_fo, s_wd, s_gt, s_ut, s_og, s_ou, s_pg, s_pu, s_h, s_dg, s_du, s_fin,
    s_psend, s_precv, s_rsend, s_rrecv, c_ring, c_part,
):
    M, D = dyb.shape[1:]
    W = wgb.shape[1] // 2
    F, FT = dg.shape[1], wdb.shape[1]
    H = M // 2
    i = lax.axis_index("tp")
    core = i % 2
    chip = i // 2
    y = chip // 4
    z = chip % 4
    r = z + y * (7 - 2 * z)
    sgn = 1 - 2 * core
    nxt = {"tp": 2 * chip_at((r + sgn + 8) % 8) + core}
    prv = {"tp": 2 * chip_at((r - sgn + 8) % 8) + core}
    par = {"tp": 2 * chip + 1 - core}
    MESH = pl.DeviceIdType.MESH

    def rows_own(h):
        return pl.multiple_of((2 * chip_at((r - sgn * (1 + h) + 16) % 8) + core) * W, W)

    def rows_par(h):
        return pl.multiple_of((2 * chip_at((r + sgn * (1 + h) + 16) % 8) + 1 - core) * W, W)

    ld = pltpu.make_async_copy

    def own_w(g):
        a, k, half = rows_own(g % 8), g % 2, pl.ds(0, W)
        return [
            ld(wg.at[pl.ds(a, W), :], wgb.at[k, half], s_og.at[k]),
            ld(wu.at[pl.ds(a, W), :], wub.at[k, half], s_ou.at[k]),
        ]

    def par_w(g):
        a, k, half = rows_par(g % 8), (g + 1) % 2, pl.ds(W, W)
        return [
            ld(wg.at[pl.ds(a, W), :], wgb.at[k, half], s_pg.at[k]),
            ld(wu.at[pl.ds(a, W), :], wub.at[k, half], s_pu.at[k]),
        ]

    def dh_place(k):
        c, j = k // TILES, k % TILES
        return pl.ds(pl.multiple_of(c * M, M), M), pl.ds(pl.multiple_of(j * FT, FT), FT)

    def dh_in(k):
        b = k % 2
        rows, cols = dh_place(k)
        return [
            ld(wd.at[cols, :], wdb.at[b], s_wd.at[b]),
            ld(gate.at[rows, cols], gtb.at[b], s_gt.at[b]),
            ld(up.at[rows, cols], utb.at[b], s_ut.at[b]),
        ]

    def dy_in(c, p):
        n = M // 4
        return ld(dy.at[pl.ds(pl.multiple_of(c * M + p * n, n), n), :], dyb.at[c % 2, pl.ds(p * n, n)], s_dy.at[p])

    def dh_out(k, dg, du):
        b = k % 2
        rows, cols = dh_place(k)
        return [
            ld(hb.at[b], hido.at[rows, cols], s_h.at[b]),
            ld(dg.at[:, cols], dguo.at[rows, cols], s_dg.at[b]),
            ld(du.at[:, cols], dguo.at[rows, pl.ds(pl.multiple_of(F + k % TILES * FT, FT), FT)], s_du.at[b]),
        ]

    def extra_in(c):
        n = extra.shape[1]
        return [
            ld(hido.at[pl.ds(c * M, M), :], dyb.at[0, :, pl.ds(c * F, F)], s_dy.at[c]),
            ld(dy.at[pl.ds(c * M, M), pl.ds(0, n)], dyb.at[1, :, pl.ds(c * n, n)], s_fd.at[c]),
        ]

    def extra_out(u):
        rows, cols = pl.ds(pl.multiple_of(u % 2 * (F // 2), F // 2), F // 2), pl.ds(pl.multiple_of(u // 2 * FT, FT), FT)
        return ld(fout.at[u % 2], extra.at[rows, cols], s_fo.at[u % 2])

    def fin(e, c):
        return ld(rsend.at[e, 2], piece.at[pl.ds(pl.multiple_of(c * M + e * H, H), H), :], s_fin.at[e])

    def ring(e, m):
        return pltpu.make_async_remote_copy(
            rsend.at[e, m % 2], rrecv.at[e, m % 3], s_rsend.at[e, m % 2], s_rrecv.at[e, m % 3], device_id=nxt, device_id_type=MESH
        )

    def part(g):
        return pltpu.make_async_remote_copy(
            psend.at[g % 2], precv.at[g % 4], s_psend.at[g % 2], s_precv.at[g % 4], device_id=par, device_id_type=MESH
        )

    def start(copies):
        for c in copies:
            c.start()

    def wait(copies):
        for c in copies:
            c.wait()

    def dh_tile(k, dg, du):
        b, cols = k % 2, dh_place(k)[1]
        d = nt(dyb[(k // TILES) % 2], wdb[b])
        g = gtb[b].astype(F32)
        u = utb[b].astype(F32)
        sig = lax.logistic(g)
        silu = g * sig
        hb[b] = (silu * u).astype(BF)
        du[:, cols] = (d * silu).astype(BF)
        dg[:, cols] = (d * u * (sig * (1.0 + g * (1.0 - sig)))).astype(BF)

    def own_tile(g):
        b, half = g % 2, pl.ds(0, W)
        term = nt(dg[...], wgb[b, half]) + nt(du[...], wub[b, half])
        own[g % 2] = term + precv[g % 4].astype(F32)

    def par_tile(g, dg, du):
        b, half = (g + 1) % 2, pl.ds(W, W)
        psend[g % 2] = (nt(dg[...], wgb[b, half]) + nt(du[...], wub[b, half])).astype(BF)

    def add(e, g, src, dst):
        total = own[g % 2, pl.ds(e * H, H)] + rrecv[e, src].astype(F32)
        rsend[e, dst] = total.astype(BF)

    def extra_piece(u):
        n, half = extra.shape[1], F // 2
        total = None
        for c in range(CHUNKS):
            h = dyb[0, :, pl.ds(pl.multiple_of(c * F + u % 2 * half, half), half)]
            d = dyb[1, :, pl.ds(pl.multiple_of(c * n + u // 2 * FT, FT), FT)]
            term = tn(h, d)
            total = term if c == 0 else total + term
        fout[u % 2] = total.astype(BF)

    def dh_ready(k, early=False):
        wait(dh_in(k))
        if early:
            pl.when(k >= 2)(lambda: wait(dh_out(k - 2, dg, du)))
        else:
            wait(dh_out(k - 2, dg, du))

    def dh_done(k, dg, du):
        start(dh_out(k, dg, du))

        @pl.when(k + 2 < CHUNKS * TILES)
        def _():
            start(dh_in(k + 2))

    start(dh_in(0))
    for p in range(4):
        dy_in(0, p).start()
    start(dh_in(1))
    start(par_w(0))
    start(own_w(0))
    start(par_w(1))
    start(own_w(1))
    barrier = pltpu.get_barrier_semaphore()
    for d in (nxt, prv, par):
        pl.semaphore_signal(barrier, inc=1, device_id=d, device_id_type=MESH)
    for e in range(2):
        rrecv[e, 3] = jnp.zeros((H, W), BF)

    @pl.loop(0, TILES)
    def _(k):
        @pl.when(k == 0)
        def _():
            for p in range(4):
                dy_in(0, p).wait()

        dh_ready(k, early=True)
        dh_tile(k, dg, du)
        dh_done(k, dg, du)

        @pl.when(k < 4)
        def _():
            dy_in(1, k).start()

    wait(par_w(0))
    par_tile(0, dg, du)
    pl.semaphore_wait(barrier, 3)
    part(0).start()
    start(par_w(2))

    @pl.loop(0, STEPS)
    def _(t):
        c, s = t // 8, t % 8
        has_dh = (s < 7) & (c < CHUNKS - 1)
        k = TILES * (c + 1) + s
        g = t - 1
        h = (g + 8) % 8
        m = 7 * ((g + 8) // 8 - 1) + h
        adds = t >= 1
        takes = adds & (h >= 1)
        sends = adds & (h <= 6)
        ends = adds & (h == 7)
        last = (h + 1) // 8
        got = (h + 7) // 8 * (1 - (STEPS - t) // STEPS)
        src = got * ((m + 2) % 3) + (1 - got) * 3
        dst = (1 - last) * (m % 2) + last * 2

        @pl.when(has_dh)
        def _():
            dh_ready(k)

        @pl.when(jnp.logical_not(has_dh))
        def _():
            wait(own_w(t))

            @pl.when(t + 1 < STEPS)
            def _():
                wait(par_w(t + 1))

        @pl.when(s == 0)
        def _():
            @pl.when(c < CHUNKS - 1)
            def _():
                for p in range(4):
                    dy_in(c + 1, p).wait()

            @pl.when(t >= 16)
            def _():
                for e in range(2):
                    fin(e, c - 2).wait()

        @pl.when(adds)
        def _():
            part(g).wait_send()

        @pl.when(sends)
        def _():
            @pl.when(m >= 2)
            def _():
                for e in range(2):
                    ring(e, m - 2).wait_send()

            @pl.when(m >= 3)
            def _():
                for e in range(2):
                    pl.semaphore_wait(c_ring.at[e], 1)

        def pass_on(e):
            @pl.when(takes)
            def _():
                ring(e, m - 1).wait_recv()

            add(e, g, src, dst)

            @pl.when(sends)
            def _():
                ring(e, m).start()

        pass_on(0)

        @pl.when(has_dh)
        def _():
            dh_tile(k, dgn, dun)

        @pl.when((s < 7) & (c == CHUNKS - 1))
        def _():
            @pl.when(s == 0)
            def _():
                for b in range(CHUNKS):
                    wait(extra_in(b))

            @pl.when(s >= 2)
            def _():
                extra_out(s - 2).wait()

            par_tile(t + 1, dg, du)
            extra_piece(s)
            extra_out(s).start()

        @pl.when((s == 7) & (c < CHUNKS - 1))
        def _():
            par_tile(t + 1, dgn, dun)

        @pl.when(t == STEPS - 1)
        def _():
            extra_out(5).wait()
            extra_piece(7)
            extra_out(7).start()

        pass_on(1)

        @pl.when(has_dh)
        def _():
            wait(own_w(t))
            wait(par_w(t + 1))
            part(t).wait_recv()
            own_tile(t)
            par_tile(t + 1, dg, du)
            dh_done(k, dgn, dun)
            start(own_w(t + 2))
            start(par_w(t + 3))

        @pl.when(jnp.logical_not(has_dh))
        def _():
            part(t).wait_recv()
            own_tile(t)

            @pl.when((s == 7) & (c < CHUNKS - 1))
            def _():
                dg[...] = dgn[...]
                du[...] = dun[...]

            @pl.when(t + 2 < STEPS)
            def _():
                start(own_w(t + 2))

            @pl.when(t + 3 < STEPS)
            def _():
                start(par_w(t + 3))

        @pl.when(ends)
        def _():
            for e in range(2):
                fin(e, c - 1).start()

        @pl.when(t + 1 < STEPS)
        def _():
            @pl.when(t >= 2)
            def _():
                pl.semaphore_wait(c_part, 1)

            part(t + 1).start()

        @pl.when(takes & (m - 1 < SENDS - 3))
        def _():
            for e in range(2):
                pl.semaphore_signal(c_ring.at[e], inc=1, device_id=prv, device_id_type=MESH)

        @pl.when(t < STEPS - 3)
        def _():
            pl.semaphore_signal(c_part, inc=1, device_id=par, device_id_type=MESH)

        @pl.when((s < 4) & (c < CHUNKS - 2))
        def _():
            dy_in(c + 2, s).start()

        @pl.when(c == CHUNKS - 2)
        def _():
            @pl.when(s == 2)
            def _():
                for b in range(CHUNKS - 1):
                    extra_in(b)[0].start()

            @pl.when(s == 6)
            def _():
                for b in range(CHUNKS):
                    extra_in(b)[1].start()

            @pl.when(s == 7)
            def _():
                for k in (CHUNKS * TILES - 2, CHUNKS * TILES - 1):
                    wait(dh_out(k, dgn, dun))
                extra_in(CHUNKS - 1)[0].start()

    part(STEPS - 1).wait_send()

    def end(e):
        fin(e, CHUNKS - 2).wait()
        ring(e, SENDS - 1).wait_recv()
        add(e, STEPS - 1, (SENDS - 1) % 3, 2)
        fin(e, CHUNKS - 1).start()

    end(0)

    @pl.loop(8, EXTRA)
    def _(u):
        extra_out(u - 2).wait()
        extra_piece(u)
        extra_out(u).start()

    end(1)
    for e in range(2):
        ring(e, SENDS - 2).wait_send()
        ring(e, SENDS - 1).wait_send()
        fin(e, CHUNKS - 1).wait()
    extra_out(EXTRA - 2).wait()
    extra_out(EXTRA - 1).wait()


def reduce_call(dy, wd, gate, up, wg, wu):
    T, D = dy.shape
    F = gate.shape[1]
    M, W, FT = T // CHUNKS, D // (2 * CHIPS), F // TILES
    hbm = pl.BlockSpec(memory_space=pltpu.HBM)
    dma, reg = pltpu.SemaphoreType.DMA, pltpu.SemaphoreType.REGULAR
    v = pltpu.VMEM
    return pl.pallas_call(
        reduce_kernel,
        in_specs=[hbm] * 6,
        out_specs=[hbm] * 4,
        out_shape=[jax.ShapeDtypeStruct(n, BF) for n in ((T, 2 * F), (T, F), (T, W), (F, EXTRA // 2 * FT))],
        scratch_shapes=[
            v((2, M, D), BF), v((2, FT, D), BF), v((2, M, FT), BF), v((2, M, FT), BF),
            v((M, F), BF), v((M, F), BF), v((M, F), BF), v((M, F), BF), v((2, M, FT), BF), v((2, 2 * W, F), BF), v((2, 2 * W, F), BF),
            v((2, M, W), F32), v((4, M, W), BF), v((2, M, W), BF), v((2, 4, M // 2, W), BF), v((2, 3, M // 2, W), BF), v((2, F // 2, FT), BF),
            dma((4,)), dma((4,)), dma((2,)), *[dma((2,))] * 11,
            dma((2,)), dma((4,)), dma((2, 2)), dma((2, 3)), reg((2,)), reg,
        ],
        compiler_params=pltpu.CompilerParams(collective_id=0, has_side_effects=True, vmem_limit_bytes=VMEM_LIMIT),
        name="dx_reduce",
    )(dy, wd, gate, up, wg, wu)


ANY = pl.BlockSpec(memory_space=pl.ANY)
RESIDENT = pl.BlockSpec(memory_space=pltpu.VMEM)


def gate_up_grads(x, dgu, extra, dw_down, bm):
    T, D = x.shape
    F = dgu.shape[1] // 2
    steps = D // bm
    n = extra.shape[1]

    def body(x_ref, d_ref, e_ref, w_ref, og, ou, ow):
        ow[...] = e_ref[...]
        both = tn(x_ref[...], d_ref[...])
        og[...] = both[:, :F].astype(BF)
        ou[...] = both[:, F:].astype(BF)

    some = pl.BlockSpec((F // steps, n), lambda i: (i, 0))
    extra = pltpu.with_memory_space_constraint(extra, pltpu.HBM)
    return pl.pallas_call(
        body,
        grid=(steps,),
        in_specs=[pl.BlockSpec((T, bm), lambda i: (0, i)), RESIDENT, some, ANY],
        out_specs=[pl.BlockSpec((bm, F), lambda i: (i, 0))] * 2 + [some],
        out_shape=[jax.ShapeDtypeStruct((D, F), BF)] * 2 + [jax.ShapeDtypeStruct((F, D), BF)],
        input_output_aliases={3: 2},
        compiler_params=pltpu.CompilerParams(vmem_limit_bytes=26 * 2**20),
        cost_estimate=pl.CostEstimate(flops=4 * T * D * F, bytes_accessed=2 * (T * D + 2 * T * F + 2 * D * F), transcendentals=0),
        name="dw_gate_up",
    )(x, dgu, extra, dw_down)


def down_kernel(lo, steps, moving, *refs):
    if moving:
        hid, dy, src, _, out, dst, hidb, dyb, ob, cb, s_h, s_d, s_o, s_in, s_out = refs
    else:
        hid, dy, out, hidb, dyb, ob, acc, s_h, s_d, s_o = refs
    ld = pltpu.make_async_copy
    T = hid.shape[0]
    bn = dyb.shape[2]
    half = T // 2

    def cols(i):
        return pl.ds(pl.multiple_of((lo + i) * bn, bn), bn)

    def h_in(p):
        rows = pl.ds(p * half, half)
        return ld(hid.at[rows, :], hidb.at[rows, :], s_h.at[p])

    def dy_in(i, p):
        rows = pl.ds(p * half, half)
        return ld(dy.at[rows, cols(i)], dyb.at[i % 2, rows], s_d.at[i % 2, p])

    def put(i):
        return ld(ob.at[i % 2], out.at[:, cols(i)], s_o.at[i % 2])

    if moving:
        n = cb.shape[1]

        def rows_at(k):
            return pl.ds(pl.multiple_of(k * n, n), n)

        def come(k):
            return ld(src.at[rows_at(k), :], cb.at[k % 8], s_in.at[k % 8])

        def go(k):
            return ld(cb.at[k % 8], dst.at[rows_at(k), :], s_out.at[k % 8])

    for p in range(2):
        h_in(p).start()
        dy_in(0, p).start()
    if moving:
        for k in range(4):
            come(k).start()
    for p in range(2):
        dy_in(1, p).start()

    def block(i):
        for p in range(2):
            dy_in(i, p).wait()

        @pl.when(i >= 2)
        def _():
            put(i - 2).wait()

        if moving:
            for e in range(2):
                come(2 * i + e).wait()
                go(2 * i + e).start()

            @pl.when(i >= 2)
            def _():
                for e in range(2):
                    go(2 * i - 4 + e).wait()

            @pl.when(i + 2 < steps)
            def _():
                for e in range(2):
                    come(2 * i + 4 + e).start()

        ob[i % 2] = tn(hidb[...], dyb[i % 2]).astype(BF)
        end(i)

    def end(i):
        put(i).start()

        @pl.when(i + 2 < steps)
        def _():
            for p in range(2):
                dy_in(i + 2, p).start()

    if moving:
        for p in range(2):
            h_in(p).wait()
        pl.loop(0, steps)(block)
        for k in range(2 * steps - 4, 2 * steps):
            go(k).wait()
    else:
        for p in range(2):
            h_in(p).wait()
            dy_in(0, p).wait()
            rows = pl.ds(p * half, half)
            term = tn(hidb[rows], dyb[0, rows])
            if p == 0:
                acc[...] = term
            else:
                ob[0] = (acc[...] + term).astype(BF)
        end(0)
        pl.loop(1, steps)(block)
    put(steps - 2).wait()
    put(steps - 1).wait()


def down_grad(hid, dy, bn, lo, hi, moved=(), prev=()):
    T, D = dy.shape
    F = hid.shape[1]
    steps = hi - lo
    hbm = pl.BlockSpec(memory_space=pltpu.HBM)
    dma, v = pltpu.SemaphoreType.DMA, pltpu.VMEM
    hid, dy = (pltpu.with_memory_space_constraint(a, pltpu.HBM) for a in (hid, dy))
    scratch = [v((T, F), BF), v((2, T, bn), BF), v((2, F, bn), BF)]
    scratch.append(v((8, T // (2 * steps), D), BF) if moved else v((F, bn), F32))
    scratch += [dma((2,)), dma((2, 2)), dma((2,))] + [dma((8,))] * (2 * len(moved))
    return pl.pallas_call(
        functools.partial(down_kernel, lo, steps, bool(moved)),
        in_specs=[hbm] * (2 + len(moved) + len(prev)),
        out_specs=[hbm] * (1 + len(moved)),
        out_shape=[jax.ShapeDtypeStruct((F, D), BF), *[jax.ShapeDtypeStruct((T, D), BF)] * len(moved)],
        scratch_shapes=scratch,
        input_output_aliases={2 + len(moved): 0} if prev else {},
        compiler_params=pltpu.CompilerParams(vmem_limit_bytes=(48 if moved else 30) * 2**20),
        cost_estimate=pl.CostEstimate(
            flops=2 * T * F * bn * steps,
            bytes_accessed=2 * (T * F + (T + F) * bn * steps + 2 * T * D * len(moved)),
            transcendentals=0,
        ),
        name="dw_down",
    )(hid, dy, *moved, *prev)


def solution(mesh):
    def step(x, dy, gate, up, w_gate, w_up, w_down):
        D = x.shape[1]
        dgu, hid, piece, extra = reduce_call(dy, w_down, gate, up, w_gate, w_up)
        gathered = lax.all_gather(piece, "tp", axis=1, tiled=True)
        bn = D // 16
        (dw_down,) = down_grad(hid, dy, bn, extra.shape[1] // bn, 12)
        dw_gate, dw_up, dw_down = gate_up_grads(x, dgu, extra, dw_down, D // 16)
        dw_down, dx = down_grad(hid, dy, bn // 2, 24, 32, (gathered,), (dw_down,))
        return dx, dw_gate, dw_up, dw_down

    tokens, columns, rows = P("dp", None), P(None, "tp"), P("tp", None)
    return jax.shard_map(
        step,
        mesh=mesh,
        in_specs=(tokens, tokens, P("dp", "tp"), P("dp", "tp"), columns, columns, rows),
        out_specs=(tokens, P("dp", "tp"), P("dp", "tp"), P(("dp", "tp"), None)),
        check_vma=False,
    )
```
